16 devices in a mesh: dp: 2 (over z), fsdp: 8 (over y, x, core).
Axes of the slice: x: 2, y: 2, z: 2, core: 2. Of those that a mesh axis runs over, the one named last changes fastest.
Arguments:
- h_saved: bfloat16 [3, 16, 2048, 896], P(None, ('dp', 'fsdp'))
- grad_out: bfloat16 [16, 2048, 896], P(('dp', 'fsdp'))
- w_gate: bfloat16 [3, 896, 4864], P(None, 'fsdp')
- w_up: bfloat16 [3, 896, 4864], P(None, 'fsdp')
- w_down: bfloat16 [3, 4864, 896], P(None, 'fsdp')
Outputs:
- output 1: float32 [3, 896, 4864], P(None, 'fsdp')
- output 2: float32 [3, 896, 4864], P(None, 'fsdp')
- output 3: float32 [3, 4864, 896], P(None, 'fsdp')
- output 4: bfloat16 [16, 2048, 896], P(('dp', 'fsdp'))
All inputs are finite; a program needn't handle non-finite values.
Results may differ from the reference program's by a relative error of at most 0.00548976.
Values are sent between devices in bfloat16 or wider.
A program may use at most 1 GiB of HBM per device.

```python
import jax
import jax.numpy as jnp
from jax import lax

LAYERS = 3
BATCH_DEV = 1
SEQ = 2048
D = 896
FF = 4864
SHARDS = 16

BATCH = SHARDS * BATCH_DEV
TOK_SHARD = BATCH_DEV * SEQ
EPS = 1e-5


def setup_inputs(seed: int = 0) -> dict:
    keys = jax.random.split(jax.random.key(seed), 5)
    h_saved = jax.random.normal(keys[0], (LAYERS, BATCH, SEQ, D), jnp.float32).astype(jnp.bfloat16)
    grad_out = jax.random.normal(keys[1], (BATCH, SEQ, D), jnp.float32).astype(jnp.bfloat16)
    w_gate = (jax.random.normal(keys[2], (LAYERS, D, FF), jnp.float32) * D ** -0.5).astype(jnp.bfloat16)
    w_up = (jax.random.normal(keys[3], (LAYERS, D, FF), jnp.float32) * D ** -0.5).astype(jnp.bfloat16)
    w_down = (jax.random.normal(keys[4], (LAYERS, FF, D), jnp.float32) * FF ** -0.5).astype(jnp.bfloat16)
    return {"h_saved": h_saved, "grad_out": grad_out, "w_gate": w_gate, "w_up": w_up, "w_down": w_down}


def layer_backward(h_in, g_acc, gate_w, up_w, down_w):
    x_full = h_in.astype(jnp.float32)
    inv_rms = lax.rsqrt(jnp.mean(x_full * x_full, axis=-1, keepdims=True) + EPS)
    norm_f = x_full * inv_rms
    norm_b = norm_f.astype(jnp.bfloat16)
    pre_gate = jnp.dot(norm_b, gate_w, preferred_element_type=jnp.float32)
    pre_up = jnp.dot(norm_b, up_w, preferred_element_type=jnp.float32)
    sig_gate = jax.nn.sigmoid(pre_gate)
    silu_gate = pre_gate * sig_gate
    act_b = (silu_gate * pre_up).astype(jnp.bfloat16)
    g_bf = g_acc.astype(jnp.bfloat16)
    d_act = jnp.dot(g_bf, down_w.T, preferred_element_type=jnp.float32)
    grad_down = jnp.dot(act_b.T, g_bf, preferred_element_type=jnp.float32)
    d_gate_b = (d_act * pre_up * sig_gate * (1.0 + pre_gate * (1.0 - sig_gate))).astype(jnp.bfloat16)
    d_up_b = (d_act * silu_gate).astype(jnp.bfloat16)
    grad_gate = jnp.dot(norm_b.T, d_gate_b, preferred_element_type=jnp.float32)
    grad_up = jnp.dot(norm_b.T, d_up_b, preferred_element_type=jnp.float32)
    d_norm = jnp.dot(d_gate_b, gate_w.T, preferred_element_type=jnp.float32) + jnp.dot(d_up_b, up_w.T, preferred_element_type=jnp.float32)
    d_x = inv_rms * (d_norm - norm_f * jnp.mean(d_norm * norm_f, axis=-1, keepdims=True))
    return g_acc + d_x, grad_gate, grad_up, grad_down


def reference(h_saved, grad_out, w_gate, w_up, w_down):
    h_blocks = h_saved.reshape(LAYERS, SHARDS, TOK_SHARD, D)
    g_init = grad_out.reshape(SHARDS, TOK_SHARD, D).astype(jnp.float32)

    def layer_step(g_all, layer_in):
        h_layer, gate_w, up_w, down_w = layer_in
        zero_in = jnp.zeros((D, FF), jnp.float32)
        zero_out = jnp.zeros((FF, D), jnp.float32)

        def shard_step(sums, shard_in):
            h_in, g_acc = shard_in
            g_next, grad_gate, grad_up, grad_down = layer_backward(h_in, g_acc, gate_w, up_w, down_w)
            return (sums[0] + grad_gate, sums[1] + grad_up, sums[2] + grad_down), g_next

        sums, g_new = lax.scan(shard_step, (zero_in, zero_in, zero_out), (h_layer, g_all))
        return g_new, sums

    g_final, grads = lax.scan(layer_step, g_init, (h_blocks, w_gate, w_up, w_down), reverse=True)
    d_h0 = g_final.reshape(BATCH, SEQ, D).astype(jnp.bfloat16)
    return grads[0], grads[1], grads[2], d_h0
```

```python
import jax
import jax.numpy as jnp
from jax import lax
from jax.experimental import pallas as pl
from jax.experimental.pallas import tpu as pltpu
from jax.sharding import PartitionSpec as P

EPS = 1e-5
MESH = pl.DeviceIdType.MESH
F32, BF16 = jnp.float32, jnp.bfloat16
L, T, D, FF = 3, 2048, 896, 4864
NJ, FC = 19, 256
NI = 10
NT = L * NI
TB = 512
UB = 256
R1, R2, R3 = 3, 3, 3
PF = 5
ND = 3
WS = 8
ORDER = (0, 4, 2, 6, 1, 3, 5, 7)


def dg(a, b, ca, cb):
    return lax.dot_general(a, b, (((ca,), (cb,)), ((), ())), preferred_element_type=F32)


def kernel(h, gout, wgu, wd, og, ou, od, dh0, wbg, wbd, dnx, gbuf,
           n_v, gb_v, dn_v, wg_v, wd_v, Gg, Gu, Gd, r1g, r1u, r1d, r2g, r2u, r2d, r3g, r3u, r3d,
           st_h, st_n, st_dnx, st_g,
           w_recv, w_send, rl_send, load_sem, s1_send, s1_recv, s2_send, s2_recv, s3_send, s3_recv,
           o_send, o_recv, x_send, x_recv, st_sem, cr1, cr2, cr3):
    z, f = lax.axis_index("dp"), lax.axis_index("fsdp")
    y, x, c = f // 4, (f // 2) % 2, f % 2

    def dev(zz, yy, xx, cc):
        return (zz, 4 * yy + 2 * xx + cc)

    xn, yn, zn = dev(z, y, 1 - x, c), dev(z, 1 - y, x, c), dev(1 - z, y, x, c)
    sib = dev(z, y, x, 1 - c)

    def rcopy(src, dst, ss, rs, to):
        return pltpu.make_async_remote_copy(src, dst, ss, rs, device_id=to, device_id_type=MESH)

    def wait_bytes(ref, sem):
        pltpu.make_async_copy(ref, ref, sem).wait()

    bar = pltpu.get_barrier_semaphore()
    for k in range(1, 16):
        g = (8 * z + f + k) % 16
        pl.semaphore_signal(bar, inc=1, device_id=(g // 8, g % 8), device_id_type=MESH)
    pl.semaphore_wait(bar, 15)

    def layer_of(t):
        return L - 1 - t // NI

    def drow(yy, xx, cc):
        return pl.multiple_of(jnp.where(cc == 0, 32 * (2 * xx + yy), 128 + 32 * (2 * yy + xx)), 32)

    def grow(yy, xx, n=224):
        return pl.ds(pl.multiple_of(224 * (2 * yy + xx), 16), n)

    def has(t, cc):
        return 2 * (t % NI) + cc < NJ

    def w_sends(t, cc):
        l, i = layer_of(t), t % NI
        j = 2 * i + cc
        sg, sd = wgu.at[l, j], wd.at[l, j]
        dgu = wbg.at[l, i, pl.ds(pl.multiple_of(112 * f, 16), 112)]
        dd = wbd.at[l, i, pl.ds(drow(y, x, c), 32)]
        direct = t < ND
        prim = jnp.logical_or(direct, t % 2 == z)
        slot = t % WS
        out = []
        for k, (to, cond) in enumerate((
            (dev(z, y, x, cc), cc != c),
            (dev(z, y, 1 - x, cc), prim),
            (dev(z, 1 - y, x, cc), prim),
            (dev(z, 1 - y, 1 - x, cc), direct),
        )):
            out.append((cond, [
                rcopy(sg, dgu, w_send.at[slot, cc, k, 0], w_recv.at[t, 2 * k], to),
                rcopy(sd, dd, w_send.at[slot, cc, k, 1], w_recv.at[t, 2 * k + 1], to),
            ]))
        return out

    def each_send(t, act):
        for cc in range(2):
            @pl.when(has(t, cc))
            def _():
                for cond, cps in w_sends(t, cc):
                    @pl.when(cond)
                    def _():
                        for cp in cps:
                            act(cp)

    def w_issue(t):
        each_send(t, lambda cp: cp.start())

    def w_drain(t):
        each_send(t, lambda cp: cp.wait_send())

    def relay(t, yy, xx, k, to, base):
        l, i = layer_of(t), t % NI
        g = wbg.at[l, i, grow(yy, xx)]
        cps = [rcopy(g, g, rl_send.at[t % 4, base], w_recv.at[t, 2 * k], to)]
        for cc in range(2):
            d = wbd.at[l, i, pl.ds(drow(yy, xx, cc), 32)]
            cps.append(rcopy(d, d, rl_send.at[t % 4, base + 1 + cc], w_recv.at[t, 2 * k + 1], to))
        return cps

    def relays1(t):
        return relay(t, y, 1 - x, 1, zn, 0) + relay(t, 1 - y, x, 2, zn, 3)

    def relays2(t):
        return relay(t, 1 - y, 1 - x, 3, zn, 9)

    def wait_kind(t, k):
        l, i = layer_of(t), t % NI
        wait_bytes(wbg.at[l, i, pl.ds(0, 224)], w_recv.at[t, 2 * k])
        wait_bytes(wbd.at[l, i, pl.ds(0, 64)], w_recv.at[t, 2 * k + 1])

    def relayed(t):
        return jnp.logical_and(t >= ND, jnp.logical_and(t < NT, has(t, c)))

    def w_relay1(t):
        @pl.when(jnp.logical_and(relayed(t), t % 2 == z))
        def _():
            wait_kind(t, 1)
            wait_kind(t, 2)
            for cp in relays1(t):
                cp.start()
            @pl.when((t // 2) % 2 == 0)
            def _():
                for cp in relay(t, y, 1 - x, 3, yn, 6):
                    cp.start()
            @pl.when((t // 2) % 2 == 1)
            def _():
                for cp in relay(t, 1 - y, x, 3, xn, 6):
                    cp.start()

    def w_relay2(t):
        @pl.when(jnp.logical_and(relayed(t), t % 2 == z))
        def _():
            wait_kind(t, 3)
            for cp in relays2(t):
                cp.start()

    def w_relay_drain(t):
        @pl.when(jnp.logical_and(relayed(t), t % 2 == z))
        def _():
            for cp in relays1(t) + relay(t, y, 1 - x, 3, yn, 6) + relays2(t):
                cp.wait_send()

    def loads(t):
        l, i = layer_of(t), t % NI
        s = t % 2
        j = 2 * i + c
        cps = []
        for q in range(4):
            qq = (q + 2 * y + x) % 4
            yy, xx = qq // 2, qq % 2
            if q == 0:
                for mine in (True, False):
                    ff = f if mine else 4 * y + 2 * x + 1 - c
                    cc = c if mine else 1 - c
                    rg, rd = pl.ds(pl.multiple_of(112 * ff, 16), 112), pl.ds(drow(y, x, cc), 32)
                    cps.append((wgu.at[l, j] if mine else wbg.at[l, i, rg], wg_v.at[s, rg]))
                    cps.append((wd.at[l, j] if mine else wbd.at[l, i, rd], wd_v.at[s, rd]))
            else:
                rg = grow(yy, xx)
                cps.append((wbg.at[l, i, rg], wg_v.at[s, rg]))
                for cc in range(2):
                    rd = pl.ds(drow(yy, xx, cc), 32)
                    cps.append((wbd.at[l, i, rd], wd_v.at[s, rd]))
        return cps

    def w_load(t):
        @pl.when(jnp.logical_and(t < NT, has(t, c)))
        def _():
            l, i = layer_of(t), t % NI
            wait_bytes(wbg.at[l, i, pl.ds(0, 112)], w_recv.at[t, 0])
            wait_bytes(wbd.at[l, i, pl.ds(0, 32)], w_recv.at[t, 1])
            @pl.when(jnp.logical_or(t < ND, t % 2 != z))
            def _():
                for k in (1, 2, 3):
                    wait_kind(t, k)
            for src, dst in loads(t):
                pltpu.make_async_copy(src, dst, load_sem.at[0 if src.shape[-1] == 512 else 1]).start()

    def w_load_wait(t):
        wait_bytes(wg_v.at[t % 2], load_sem.at[0])
        wait_bytes(wd_v.at[t % 2], load_sem.at[1])

    for t in range(PF):
        w_issue(jnp.int32(t))

    own0 = T * c
    oth0 = T * (1 - c)

    def rows(base, b):
        return pl.ds(pl.multiple_of(base + b * UB, UB), UB)

    def norm_block(xf):
        r = lax.rsqrt(jnp.mean(xf * xf, axis=-1, keepdims=True) + EPS)
        return r, xf * r

    gl = pltpu.make_async_copy(gout, gb_v.at[pl.ds(pl.multiple_of(own0, T), T)], st_sem.at[0])
    gr = rcopy(gout, gb_v.at[pl.ds(pl.multiple_of(own0, T), T)], x_send.at[0], x_recv.at[0], sib)
    gl.start()
    gr.start()

    NB = T // UB

    def first_blocks(b, _):
        s = b % 2
        cp = pltpu.make_async_copy(h.at[L - 1, pl.ds(pl.multiple_of(b * UB, UB), UB)], st_n.at[s], st_sem.at[3])
        cp.start()
        cp.wait()
        _, nf = norm_block(st_n[s].astype(F32))
        n_v[rows(own0, b), :] = nf.astype(BF16)
        rcopy(n_v.at[rows(own0, b)], n_v.at[rows(own0, b)], x_send.at[1], x_recv.at[1], sib).start()
        return 0

    lax.fori_loop(0, NB, first_blocks, 0)

    def half(base):
        return pl.ds(pl.multiple_of(base, T), T)

    def exchange_done():
        wait_bytes(n_v.at[half(oth0)], x_recv.at[1])
        wait_bytes(gb_v.at[half(oth0)], x_recv.at[0])
        wait_bytes(n_v.at[half(own0)], x_send.at[1])
        wait_bytes(gb_v.at[half(own0)], x_send.at[0])

    gl.wait()
    w_load(jnp.int32(0))
    exchange_done()

    def compute(s, n):
        i = s % NI
        ws, gs = s % 2, n % 2
        w_load_wait(s)
        wg, wdd = wg_v.at[ws], wd_v.at[ws]

        def block(b, _):
            rw = pl.ds(pl.multiple_of(b * TB, TB), TB)
            nb, gbb = n_v[rw, :], gb_v[rw, :]
            uv = dg(nb, wg[...], 1, 0)
            u, v = uv[:, :FC], uv[:, FC:]
            da = dg(gbb, wdd[...], 1, 1)
            sg = jax.nn.sigmoid(u)
            sl = u * sg
            a = (sl * v).astype(BF16)
            du = (da * v * sg * (1.0 + u * (1.0 - sg))).astype(BF16)
            dv = (da * sl).astype(BF16)
            duv = jnp.concatenate([du, dv], axis=1)
            dnb = dg(duv, wg[...], 1, 1)

            @pl.when(i == 0)
            def _():
                dn_v[rw, :] = dnb

            @pl.when(i > 0)
            def _():
                dn_v[rw, :] += dnb

            g2 = dg(nb, duv, 0, 0)
            g3 = dg(a, gbb, 0, 0).reshape(8, 32, D)

            def put(add):
                for q in range(4):
                    yy, xx = q // 2, q % 2
                    pg, pu = g2[224 * q:224 * q + 224, :FC], g2[224 * q:224 * q + 224, FC:]
                    if add:
                        Gg[gs, 2 * xx + yy] += pg
                        Gu[gs, q] += pu
                    else:
                        Gg[gs, 2 * xx + yy] = pg
                        Gu[gs, q] = pu
                if add:
                    Gd[gs] += g3
                else:
                    Gd[gs] = g3

            @pl.when(b == 0)
            def _():
                put(False)

            @pl.when(b > 0)
            def _():
                put(True)

            return 0

        lax.fori_loop(0, 2 * T // TB, block, 0)

    def num(s):
        return s - c * (s // NI)

    def valid(s):
        return jnp.logical_and(jnp.logical_and(s >= 0, s < NT), 2 * (s % NI) + c < NJ)

    def s1(n):
        gs, rs, k = n % 2, n % R1, n % 2
        return [
            rcopy(Gg.at[gs, pl.ds(2 * (1 - x), 2)], r1g.at[rs], s1_send.at[k, 0], s1_recv.at[rs, 0], xn),
            rcopy(Gd.at[gs, pl.ds(2 * (1 - x), 2)], r1d.at[rs, pl.ds(0, 2)], s1_send.at[k, 1], s1_recv.at[rs, 1], xn),
            rcopy(Gu.at[gs, pl.ds(2 * (1 - y), 2)], r1u.at[rs], s1_send.at[k, 2], s1_recv.at[rs, 2], yn),
            rcopy(Gd.at[gs, pl.ds(4 + 2 * (1 - y), 2)], r1d.at[rs, pl.ds(2, 2)], s1_send.at[k, 3], s1_recv.at[rs, 3], yn),
        ]

    def s2(n):
        rs, qs, k = n % R1, n % R2, n % 2
        return [
            rcopy(r1g.at[rs, 1 - y], r2g.at[qs], s2_send.at[k, 0], s2_recv.at[qs, 0], yn),
            rcopy(r1d.at[rs, 1 - y], r2d.at[qs, 0], s2_send.at[k, 1], s2_recv.at[qs, 1], yn),
            rcopy(r1u.at[rs, 1 - x], r2u.at[qs], s2_send.at[k, 2], s2_recv.at[qs, 2], xn),
            rcopy(r1d.at[rs, 3 - x], r2d.at[qs, 1], s2_send.at[k, 3], s2_recv.at[qs, 3], xn),
        ]

    def s3(n):
        qs, ps, k = n % R2, n % R3, n % 2
        return [
            rcopy(r2g.at[qs], r3g.at[ps], s3_send.at[k, 0], s3_recv.at[ps, 0], zn),
            rcopy(r2u.at[qs], r3u.at[ps], s3_send.at[k, 1], s3_recv.at[ps, 1], zn),
            rcopy(r2d.at[qs], r3d.at[ps], s3_send.at[k, 2], s3_recv.at[ps, 2], zn),
        ]

    def outs(s, n):
        l, j = layer_of(s), 2 * (s % NI) + c
        ps, k = n % R3, n % 2
        mine, other = pl.ds(pl.multiple_of(112 * c, 8), 112), pl.ds(pl.multiple_of(112 * (1 - c), 8), 112)
        local = [
            pltpu.make_async_copy(r3g.at[ps, mine], og.at[l, j], o_send.at[k, 0]),
            pltpu.make_async_copy(r3u.at[ps, mine], ou.at[l, j], o_send.at[k, 1]),
            pltpu.make_async_copy(r3d.at[ps, c], od.at[l, j], o_send.at[k, 2]),
        ]
        remote = [
            rcopy(r3g.at[ps, other], og.at[l, j], o_send.at[k, 3], o_recv.at[0], sib),
            rcopy(r3u.at[ps, other], ou.at[l, j], o_send.at[k, 4], o_recv.at[1], sib),
            rcopy(r3d.at[ps, 1 - c], od.at[l, j], o_send.at[k, 5], o_recv.at[2], sib),
        ]
        return local + remote

    def credit(sem, to):
        pl.semaphore_signal(sem, inc=1, device_id=to, device_id_type=MESH)

    def stage1(s):
        @pl.when(valid(s))
        def _():
            n = num(s)
            @pl.when(n >= R1)
            def _():
                pl.semaphore_wait(cr1.at[0], 1)
                pl.semaphore_wait(cr1.at[1], 1)
            for cp in s1(n):
                cp.start()

    last = NT - L * c

    def stage2(s):
        @pl.when(valid(s))
        def _():
            n = num(s)
            gs, rs = n % 2, n % R1
            for cp in s1(n):
                cp.wait_recv()
            r1g[rs] += Gg[gs, pl.ds(2 * x, 2)]
            r1u[rs] += Gu[gs, pl.ds(2 * y, 2)]
            r1d[rs, 0:2] += Gd[gs, pl.ds(2 * x, 2)]
            r1d[rs, 2:4] += Gd[gs, pl.ds(4 + 2 * y, 2)]
            @pl.when(n >= R2)
            def _():
                pl.semaphore_wait(cr2.at[0], 1)
                pl.semaphore_wait(cr2.at[1], 1)
            for cp in s2(n):
                cp.start()

    def stage3(s):
        @pl.when(valid(s))
        def _():
            n = num(s)
            rs, qs = n % R1, n % R2
            for cp in s2(n):
                cp.wait_recv()
            r2g[qs] += r1g[rs, y]
            r2u[qs] += r1u[rs, x]
            r2d[qs, 0] += r1d[rs, y]
            r2d[qs, 1] += r1d[rs, 2 + x]
            @pl.when(n >= R3)
            def _():
                pl.semaphore_wait(cr3, 1)
            for cp in s3(n):
                cp.start()
            for cp in s2(n):
                cp.wait_send()
            @pl.when(n + R1 < last)
            def _():
                credit(cr1.at[0], xn)
                credit(cr1.at[1], yn)

    def stage4(s):
        @pl.when(valid(s))
        def _():
            n = num(s)
            qs, ps = n % R2, n % R3
            for cp in s3(n):
                cp.wait_recv()
            r3g[ps] += r2g[qs]
            r3u[ps] += r2u[qs]
            r3d[ps] += r2d[qs]
            for cp in outs(s, n):
                cp.start()
            for cp in s3(n):
                cp.wait_send()
            @pl.when(n + R2 < last)
            def _():
                credit(cr2.at[0], yn)
                credit(cr2.at[1], xn)

    def stage5(s):
        @pl.when(valid(s))
        def _():
            n = num(s)
            cps = outs(s, n)
            for cp in cps[:3]:
                cp.wait()
            for cp in cps[3:]:
                cp.wait_send()
            @pl.when(n + R3 < last)
            def _():
                credit(cr3, zn)

    def free_g(s):
        @pl.when(valid(s))
        def _():
            for cp in s1(num(s)):
                cp.wait_send()

    def dn_copy(b):
        return rcopy(dn_v.at[rows(oth0, b)], dnx.at[pl.ds(b * UB, UB)], x_send.at[2], x_recv.at[2 + b], sib)

    def dn_send():
        for b in range(NB):
            dn_copy(b).start()

    def boundary(s):
        l = layer_of(s)

        def fetch(b):
            r = pl.ds(pl.multiple_of(b * UB, UB), UB)
            pltpu.make_async_copy(h.at[l, r], st_h, st_sem.at[1]).start()
            @pl.when(l > 0)
            def _():
                pltpu.make_async_copy(h.at[jnp.maximum(l - 1, 0), r], st_n.at[0], st_sem.at[3]).start()
            @pl.when(l < L - 1)
            def _():
                pltpu.make_async_copy(gbuf.at[r], st_g, st_sem.at[2]).start()

        def block(b, _):
            r = pl.ds(pl.multiple_of(b * UB, UB), UB)
            ro = rows(own0, b)
            fetch(b)
            wait_bytes(dnx.at[r], x_recv.at[2 + b])
            pltpu.make_async_copy(dnx.at[r], st_dnx, st_sem.at[4]).start()
            wait_bytes(st_h, st_sem.at[1])
            @pl.when(l < L - 1)
            def _():
                wait_bytes(st_g, st_sem.at[2])
            @pl.when(l == L - 1)
            def _():
                st_g[...] = gb_v[ro, :].astype(F32)
            wait_bytes(st_dnx, st_sem.at[4])
            rr, nf = norm_block(st_h[...].astype(F32))
            dn = dn_v[ro, :] + st_dnx[...]
            m = jnp.mean(dn * nf, axis=-1, keepdims=True)
            g = st_g[...] + rr * (dn - nf * m)
            gb_v[ro, :] = g.astype(BF16)

            @pl.when(l > 0)
            def _():
                st_g[...] = g
                cg = pltpu.make_async_copy(st_g, gbuf.at[r], st_sem.at[5])
                cg.start()
                rcopy(gb_v.at[ro], gb_v.at[ro], x_send.at[0], x_recv.at[0], sib).start()
                wait_bytes(st_n.at[0], st_sem.at[3])
                _, nf2 = norm_block(st_n[0].astype(F32))
                n_v[ro, :] = nf2.astype(BF16)
                rcopy(n_v.at[ro], n_v.at[ro], x_send.at[1], x_recv.at[1], sib).start()
                cg.wait()

            @pl.when(l == 0)
            def _():
                pltpu.make_async_copy(gb_v.at[ro], dh0.at[r], st_sem.at[6]).start()
            return 0

        lax.fori_loop(0, NB, block, 0)
        wait_bytes(dn_v.at[half(oth0)], x_send.at[2])

        @pl.when(l > 0)
        def _():
            exchange_done()

        @pl.when(l == 0)
        def _():
            wait_bytes(dh0, st_sem.at[6])

    def step(s, _):
        edge = jnp.logical_and(s % NI == NI - 1, s < NT)

        @pl.when(valid(s))
        def _():
            compute(s, num(s))

        stage1(s)

        @pl.when(edge)
        def _():
            dn_send()

        @pl.when(s + PF < NT)
        def _():
            @pl.when(s + PF >= WS)
            def _():
                w_drain(s + PF - WS)
            w_issue(s + PF)

        w_relay1(s + 3)
        stage2(s - 1)
        w_relay2(s + 2)
        stage3(s - 2)
        w_load(s + 1)
        stage4(s - 3)
        stage5(s - 4)
        free_g(s - 1)
        w_relay_drain(s + 1)

        @pl.when(edge)
        def _():
            boundary(s)
        return 0

    lax.fori_loop(0, NT + 4, step, 0)
    for t in range(NT - WS, NT):
        w_drain(jnp.int32(t))

    def out_done(cnt):
        wait_bytes(og.at[:, pl.ds(0, cnt)], o_recv.at[0])
        wait_bytes(ou.at[:, pl.ds(0, cnt)], o_recv.at[1])
        wait_bytes(od.at[:, pl.ds(0, cnt)], o_recv.at[2])

    @pl.when(c == 0)
    def _():
        out_done(9)

    @pl.when(c == 1)
    def _():
        out_done(10)


def call(h, gout, wgu, wd):
    A = pl.BlockSpec(memory_space=pl.ANY)
    V, S = pltpu.VMEM, pltpu.SemaphoreType
    sd = jax.ShapeDtypeStruct
    return pl.pallas_call(
        kernel,
        out_shape=(
            sd((L, NJ, 112, FC), F32), sd((L, NJ, 112, FC), F32), sd((L, NJ, 32, D), F32), sd((T, D), BF16),
            sd((L, NI, D, 2 * FC), BF16), sd((L, NI, FC, D), BF16), sd((T, D), F32), sd((T, D), F32),
        ),
        in_specs=[A] * 4,
        out_specs=(A,) * 8,
        scratch_shapes=[
            V((2 * T, D), BF16), V((2 * T, D), BF16), V((2 * T, D), F32),
            V((2, D, 2 * FC), BF16), V((2, FC, D), BF16),
            V((2, 4, 224, FC), F32), V((2, 4, 224, FC), F32), V((2, 8, 32, D), F32),
            V((R1, 2, 224, FC), F32), V((R1, 2, 224, FC), F32), V((R1, 4, 32, D), F32),
            V((R2, 224, FC), F32), V((R2, 224, FC), F32), V((R2, 2, 32, D), F32),
            V((R3, 224, FC), F32), V((R3, 224, FC), F32), V((R3, 2, 32, D), F32),
            V((UB, D), BF16), V((2, UB, D), BF16), V((UB, D), F32), V((UB, D), F32),
            S.DMA((NT, 8)), S.DMA((WS, 2, 4, 2)), S.DMA((4, 12)), S.DMA((2,)),
            S.DMA((2, 4)), S.DMA((R1, 4)), S.DMA((2, 4)), S.DMA((R2, 4)), S.DMA((2, 3)), S.DMA((R3, 3)),
            S.DMA((2, 6)), S.DMA((3,)), S.DMA((3,)), S.DMA((2 + T // UB,)), S.DMA((7,)),
            S.REGULAR((2,)), S.REGULAR((2,)), S.REGULAR,
        ],
        compiler_params=pltpu.CompilerParams(
            collective_id=0, has_side_effects=True, vmem_limit_bytes=67043328
        ),
    )(h, gout, wgu, wd)[:4]


def solution(mesh):
    tok = P(("dp", "fsdp"))
    stack = P(None, ("dp", "fsdp"))
    wsp = P(None, "fsdp")
    inv = tuple(ORDER.index(k) for k in range(8))

    def local(h, gout, wg, wu, wd):
        def pack(w):
            w = w.reshape(L, 112, 8, NJ, 32)
            w = jnp.stack([w[:, :, k] for k in ORDER], axis=3)
            return jnp.moveaxis(w, 1, 2).reshape(L, NJ, 112, FC)

        def unpack(g):
            g = g.reshape(L, NJ, 112, 8, 32)
            g = jnp.stack([g[:, :, :, k] for k in inv], axis=2)
            return jnp.transpose(g, (0, 3, 2, 1, 4)).reshape(L, 112, FF)

        wgu = jnp.concatenate([pack(wg), pack(wu)], axis=-1)
        og, ou, od, dh = call(h.reshape(L, T, D), gout.reshape(T, D), wgu, wd.reshape(L, NJ, 32, D))
        return unpack(og), unpack(ou), od.reshape(L, 608, D), dh.reshape(1, T, D)

    return jax.shard_map(
        local, mesh=mesh, in_specs=(stack, tok, wsp, wsp, wsp), out_specs=(wsp, wsp, wsp, tok), check_vma=False
    )
```

```python
import jax
import jax.numpy as jnp
from jax import lax
from jax.experimental import pallas as pl
from jax.experimental.pallas import tpu as pltpu
from jax.sharding import PartitionSpec as P

EPS = 1e-5
MESH = pl.DeviceIdType.MESH
F32, BF16 = jnp.float32, jnp.bfloat16
L, T, D, FF = 3, 2048, 896, 4864
NJ, FC = 19, 256
NI = 10
NT = L * NI
TB, UNROLL = 512, 2
UB = 128
K2, K3, K4 = 3, 6, 8
PF = 10
ND = 2
WS = 16
RS = 16
ORDER = (0, 4, 2, 6, 1, 3, 5, 7)


def dg(a, b, ca, cb):
    return lax.dot_general(a, b, (((ca,), (cb,)), ((), ())), preferred_element_type=F32)


def kernel(h, gout, wgu, wd, og, ou, od, dh0, wbg, wbd, dnx, gbuf,
           hgg, hgu, hgd, h1g, h1u, h1d, p2g, p2u, p2d, h2g, h2u, h2d, p3g, p3u, p3d, h3g, h3u, h3d,
           n_v, gb_v, dn_v, wg_v, wd_v, Gg, Gu, Gd, vg, vu, vd, st_h, st_n, st_dnx, st_g,
           w_recv, w_send, rl_send, load_sem, g_sem, v_sem, p_sem,
           s1_send, s1_recv, s2_send, s2_recv, s3_send, s3_recv,
           o_send, o_recv, x_send, x_recv, st_sem, g_st):
    z, f = lax.axis_index("dp"), lax.axis_index("fsdp")
    y, x, c = f // 4, (f // 2) % 2, f % 2

    def dev(zz, yy, xx, cc):
        return (zz, 4 * yy + 2 * xx + cc)

    xn, yn, zn = dev(z, y, 1 - x, c), dev(z, 1 - y, x, c), dev(1 - z, y, x, c)
    sib = dev(z, y, x, 1 - c)

    def rcopy(src, dst, ss, rs, to):
        return pltpu.make_async_remote_copy(src, dst, ss, rs, device_id=to, device_id_type=MESH)

    def wait_bytes(ref, sem):
        pltpu.make_async_copy(ref, ref, sem).wait()

    bar = pltpu.get_barrier_semaphore()
    for k in range(1, 16):
        g = (8 * z + f + k) % 16
        pl.semaphore_signal(bar, inc=1, device_id=(g // 8, g % 8), device_id_type=MESH)
    pl.semaphore_wait(bar, 15)

    def layer_of(t):
        return L - 1 - t // NI

    def drow(yy, xx, cc):
        return pl.multiple_of(jnp.where(cc == 0, 32 * (2 * xx + yy), 128 + 32 * (2 * yy + xx)), 32)

    def grow(yy, xx, n=224):
        return pl.ds(pl.multiple_of(224 * (2 * yy + xx), 16), n)

    def has(t, cc):
        return 2 * (t % NI) + cc < NJ

    def w_sends(t, cc):
        l, i = layer_of(t), t % NI
        j = 2 * i + cc
        sg, sd = wgu.at[l, j], wd.at[l, j]
        dgu = wbg.at[l, i, pl.ds(pl.multiple_of(112 * f, 16), 112)]
        dd = wbd.at[l, i, pl.ds(drow(y, x, c), 32)]
        direct = t < ND
        prim = jnp.logical_or(direct, t % 2 == z)
        slot = t % WS
        out = []
        for k, (to, cond) in enumerate((
            (dev(z, y, x, cc), cc != c),
            (dev(z, y, 1 - x, cc), prim),
            (dev(z, 1 - y, x, cc), prim),
            (dev(z, 1 - y, 1 - x, cc), direct),
        )):
            out.append((cond, [
                rcopy(sg, dgu, w_send.at[slot, cc, k, 0], w_recv.at[t, 2 * k], to),
                rcopy(sd, dd, w_send.at[slot, cc, k, 1], w_recv.at[t, 2 * k + 1], to),
            ]))
        return out

    def each_send(t, act):
        for cc in range(2):
            @pl.when(has(t, cc))
            def _():
                for cond, cps in w_sends(t, cc):
                    @pl.when(cond)
                    def _():
                        for cp in cps:
                            act(cp)

    def w_issue(t):
        each_send(t, lambda cp: cp.start())

    def w_drain(t):
        each_send(t, lambda cp: cp.wait_send())

    def relay(t, yy, xx, k, to, base):
        l, i = layer_of(t), t % NI
        g = wbg.at[l, i, grow(yy, xx)]
        cps = [rcopy(g, g, rl_send.at[t % RS, base], w_recv.at[t, 2 * k], to)]
        for cc in range(2):
            d = wbd.at[l, i, pl.ds(drow(yy, xx, cc), 32)]
            cps.append(rcopy(d, d, rl_send.at[t % RS, base + 1 + cc], w_recv.at[t, 2 * k + 1], to))
        return cps

    def relays1(t):
        return relay(t, y, 1 - x, 1, zn, 0) + relay(t, 1 - y, x, 2, zn, 3)

    def relays2(t):
        return relay(t, 1 - y, 1 - x, 3, zn, 9)

    def wait_kind(t, k):
        l, i = layer_of(t), t % NI
        wait_bytes(wbg.at[l, i, pl.ds(0, 224)], w_recv.at[t, 2 * k])
        wait_bytes(wbd.at[l, i, pl.ds(0, 64)], w_recv.at[t, 2 * k + 1])

    def relayed(t):
        return jnp.logical_and(t >= ND, jnp.logical_and(t < NT, has(t, c)))

    def w_relay1(t):
        @pl.when(jnp.logical_and(relayed(t), t % 2 == z))
        def _():
            wait_kind(t, 1)
            wait_kind(t, 2)
            for cp in relays1(t):
                cp.start()
            @pl.when((t // 2) % 2 == 0)
            def _():
                for cp in relay(t, y, 1 - x, 3, yn, 6):
                    cp.start()
            @pl.when((t // 2) % 2 == 1)
            def _():
                for cp in relay(t, 1 - y, x, 3, xn, 6):
                    cp.start()

    def w_relay2(t):
        @pl.when(jnp.logical_and(relayed(t), t % 2 == z))
        def _():
            wait_kind(t, 3)
            for cp in relays2(t):
                cp.start()

    def w_relay_drain(t):
        @pl.when(jnp.logical_and(relayed(t), t % 2 == z))
        def _():
            for cp in relays1(t) + relay(t, y, 1 - x, 3, yn, 6) + relays2(t):
                cp.wait_send()

    def loads(t):
        l, i = layer_of(t), t % NI
        s = t % 2
        j = 2 * i + c
        cps = []
        for q in range(4):
            qq = (q + 2 * y + x) % 4
            yy, xx = qq // 2, qq % 2
            if q == 0:
                for mine in (True, False):
                    ff = f if mine else 4 * y + 2 * x + 1 - c
                    cc = c if mine else 1 - c
                    rg, rd = pl.ds(pl.multiple_of(112 * ff, 16), 112), pl.ds(drow(y, x, cc), 32)
                    cps.append((wgu.at[l, j] if mine else wbg.at[l, i, rg], wg_v.at[s, rg]))
                    cps.append((wd.at[l, j] if mine else wbd.at[l, i, rd], wd_v.at[s, rd]))
            else:
                rg = grow(yy, xx)
                cps.append((wbg.at[l, i, rg], wg_v.at[s, rg]))
                for cc in range(2):
                    rd = pl.ds(drow(yy, xx, cc), 32)
                    cps.append((wbd.at[l, i, rd], wd_v.at[s, rd]))
        return cps

    def w_load(t):
        @pl.when(jnp.logical_and(t < NT, has(t, c)))
        def _():
            l, i = layer_of(t), t % NI
            wait_bytes(wbg.at[l, i, pl.ds(0, 112)], w_recv.at[t, 0])
            wait_bytes(wbd.at[l, i, pl.ds(0, 32)], w_recv.at[t, 1])
            @pl.when(jnp.logical_or(t < ND, t % 2 != z))
            def _():
                for k in (1, 2, 3):
                    wait_kind(t, k)
            for src, dst in loads(t):
                pltpu.make_async_copy(src, dst, load_sem.at[0 if src.shape[-1] == 512 else 1]).start()

    def w_load_wait(t):
        wait_bytes(wg_v.at[t % 2], load_sem.at[0])
        wait_bytes(wd_v.at[t % 2], load_sem.at[1])

    for t in range(PF):
        w_issue(jnp.int32(t))

    own0 = T * c
    oth0 = T * (1 - c)

    def rows(base, b):
        return pl.ds(pl.multiple_of(base + b * UB, UB), UB)

    def norm_block(xf):
        r = lax.rsqrt(jnp.mean(xf * xf, axis=-1, keepdims=True) + EPS)
        return r, xf * r

    gl = pltpu.make_async_copy(gout, gb_v.at[pl.ds(pl.multiple_of(own0, T), T)], g_st.at[0])
    gr = rcopy(gout, gb_v.at[pl.ds(pl.multiple_of(own0, T), T)], x_send.at[0], x_recv.at[0], sib)
    gl.start()
    gr.start()

    NB = T // UB

    def h_copy(b):
        return pltpu.make_async_copy(h.at[L - 1, pl.ds(pl.multiple_of(b * UB, UB), UB)], st_n.at[b % 2], st_sem.at[2, b % 2])

    h_copy(jnp.int32(0)).start()

    def first_blocks(b, _):
        @pl.when(b + 1 < NB)
        def _():
            h_copy(b + 1).start()
        h_copy(b).wait()
        _, nf = norm_block(st_n[b % 2].astype(F32))
        ro = rows(own0, b)
        n_v[ro, :] = nf.astype(BF16)
        rcopy(n_v.at[ro], n_v.at[ro], x_send.at[1], x_recv.at[1], sib).start()
        return 0

    lax.fori_loop(0, NB, first_blocks, 0)

    def half(base):
        return pl.ds(pl.multiple_of(base, T), T)

    def exchange_done():
        wait_bytes(n_v.at[half(oth0)], x_recv.at[1])
        wait_bytes(gb_v.at[half(oth0)], x_recv.at[0])
        wait_bytes(n_v.at[half(own0)], x_send.at[1])
        wait_bytes(gb_v.at[half(own0)], x_send.at[0])

    gl.wait()
    w_load(jnp.int32(0))
    exchange_done()

    def compute(s):
        i = s % NI
        ws = s % 2
        w_load_wait(s)
        wg, wdd = wg_v.at[ws], wd_v.at[ws]

        def block(b, _):
            def load(k):
                rw = pl.ds(pl.multiple_of((b * UNROLL + k) * TB, TB), TB)
                return rw, n_v[rw, :], gb_v[rw, :]

            def first(k):
                _, nb, gbb = load(k)
                return dg(nb, wg[...], 1, 0), dg(gbb, wdd[...], 1, 1)

            def middle(uv, da):
                u, v = uv[:, :FC], uv[:, FC:]
                sg = jax.nn.sigmoid(u)
                sl = u * sg
                a = (sl * v).astype(BF16)
                du = (da * v * sg * (1.0 + u * (1.0 - sg))).astype(BF16)
                dv = (da * sl).astype(BF16)
                return a, jnp.concatenate([du, dv], axis=1)

            def second(k, a, duv):
                rw, nb, gbb = load(k)
                dnb = dg(duv, wg[...], 1, 1)
                dn_v[rw, :] = jnp.where(i == 0, 0.0, dn_v[rw, :]) + dnb
                g2 = dg(nb, duv, 0, 0)
                g3 = dg(a, gbb, 0, 0).reshape(8, 32, D)

                def old(ref):
                    return jnp.where(b == 0, 0.0, ref[...]) if k == 0 else ref[...]

                for q in range(4):
                    yy, xx = q // 2, q % 2
                    rg, ru = Gg.at[2 * xx + yy], Gu.at[q]
                    rg[...] = old(rg) + g2[224 * q:224 * q + 224, :FC]
                    ru[...] = old(ru) + g2[224 * q:224 * q + 224, FC:]
                Gd[...] = old(Gd) + g3

            mids = [middle(*first(k)) for k in range(UNROLL)]
            for k in range(UNROLL):
                second(k, *mids[k])
            return 0

        lax.fori_loop(0, 2 * T // (TB * UNROLL), block, 0)

    def valid(s):
        return jnp.logical_and(jnp.logical_and(s >= 0, s < NT), 2 * (s % NI) + c < NJ)

    def when_valid(s):
        return pl.when(valid(s))

    def s1(s):
        ax, ay = pl.ds(2 * (1 - x), 2), pl.ds(2 * (1 - y), 2)
        by = pl.ds(4 + 2 * (1 - y), 2)
        return [
            rcopy(hgg.at[s, ax], h1g.at[s], s1_send.at[s, 0], s1_recv.at[s, 0], xn),
            rcopy(hgd.at[s, ax], h1d.at[s, pl.ds(0, 2)], s1_send.at[s, 1], s1_recv.at[s, 1], xn),
            rcopy(hgu.at[s, ay], h1u.at[s], s1_send.at[s, 2], s1_recv.at[s, 2], yn),
            rcopy(hgd.at[s, by], h1d.at[s, pl.ds(2, 2)], s1_send.at[s, 3], s1_recv.at[s, 3], yn),
        ]

    def s2(s):
        return [
            rcopy(p2g.at[s], h2g.at[s], s2_send.at[s, 0], s2_recv.at[s, 0], yn),
            rcopy(p2d.at[s, 0], h2d.at[s, 0], s2_send.at[s, 1], s2_recv.at[s, 1], yn),
            rcopy(p2u.at[s], h2u.at[s], s2_send.at[s, 2], s2_recv.at[s, 2], xn),
            rcopy(p2d.at[s, 1], h2d.at[s, 1], s2_send.at[s, 3], s2_recv.at[s, 3], xn),
        ]

    def s3(s):
        return [
            rcopy(p3g.at[s], h3g.at[s], s3_send.at[s, 0], s3_recv.at[s, 0], zn),
            rcopy(p3u.at[s], h3u.at[s], s3_send.at[s, 1], s3_recv.at[s, 1], zn),
            rcopy(p3d.at[s], h3d.at[s], s3_send.at[s, 2], s3_recv.at[s, 2], zn),
        ]

    def outs(s):
        l, j = layer_of(s), 2 * (s % NI) + c
        mine, other = pl.ds(pl.multiple_of(112 * c, 8), 112), pl.ds(pl.multiple_of(112 * (1 - c), 8), 112)
        local = [
            pltpu.make_async_copy(vg.at[5, mine], og.at[l, j], o_send.at[0]),
            pltpu.make_async_copy(vu.at[5, mine], ou.at[l, j], o_send.at[1]),
            pltpu.make_async_copy(vd.at[5, c], od.at[l, j], o_send.at[2]),
        ]
        remote = [
            rcopy(vg.at[5, other], og.at[l, j], o_send.at[3], o_recv.at[0], sib),
            rcopy(vu.at[5, other], ou.at[l, j], o_send.at[4], o_recv.at[1], sib),
            rcopy(vd.at[5, 1 - c], od.at[l, j], o_send.at[5], o_recv.at[2], sib),
        ]
        return local + remote

    def fetch(slot, g, u, d0, d1):
        pltpu.make_async_copy(g, vg.at[slot], v_sem.at[slot, 0]).start()
        pltpu.make_async_copy(u, vu.at[slot], v_sem.at[slot, 1]).start()
        pltpu.make_async_copy(d0, vd.at[slot, 0], v_sem.at[slot, 2]).start()
        pltpu.make_async_copy(d1, vd.at[slot, 1], v_sem.at[slot, 3]).start()

    def fetched(*slots):
        for k in slots:
            wait_bytes(vg.at[k], v_sem.at[k, 0])
            wait_bytes(vu.at[k], v_sem.at[k, 1])
            wait_bytes(vd.at[k, 0], v_sem.at[k, 2])
            wait_bytes(vd.at[k, 1], v_sem.at[k, 3])

    def add(slot, *more):
        for r in (vg, vu, vd):
            t = r[slot]
            for k in more:
                t = t + r[k]
            r[slot] = t

    def arrive(cps):
        for cp in cps:
            cp.wait_recv()

    def begin(s):
        m2, m3, m4 = s - K2, s - K3, s - K4

        @when_valid(m4 - 1)
        def _():
            cps = outs(m4 - 1)
            for cp in cps[:3]:
                cp.wait()
            for cp in cps[3:]:
                cp.wait_send()

        @when_valid(m2)
        def _():
            arrive(s1(m2))
            fetch(0, hgg.at[m2, 2 * x + 1 - y], hgu.at[m2, 2 * y + 1 - x], hgd.at[m2, 2 * x + 1 - y], hgd.at[m2, 4 + 2 * y + 1 - x])
            fetch(1, h1g.at[m2, 1 - y], h1u.at[m2, 1 - x], h1d.at[m2, 1 - y], h1d.at[m2, 3 - x])

        @when_valid(m3)
        def _():
            arrive(s2(m3))
            fetch(2, hgg.at[m3, 2 * x + y], hgu.at[m3, 2 * y + x], hgd.at[m3, 2 * x + y], hgd.at[m3, 4 + 2 * y + x])
            fetch(3, h1g.at[m3, y], h1u.at[m3, x], h1d.at[m3, y], h1d.at[m3, 2 + x])
            fetch(4, h2g.at[m3], h2u.at[m3], h2d.at[m3, 0], h2d.at[m3, 1])

        @when_valid(m4)
        def _():
            arrive(s3(m4))
            fetch(5, p3g.at[m4], p3u.at[m4], p3d.at[m4, 0], p3d.at[m4, 1])
            fetch(6, h3g.at[m4], h3u.at[m4], h3d.at[m4, 0], h3d.at[m4, 1])

    def put(slot, k, g, u, d):
        return [
            pltpu.make_async_copy(vg.at[slot], g, p_sem.at[k, 0]),
            pltpu.make_async_copy(vu.at[slot], u, p_sem.at[k, 1]),
            pltpu.make_async_copy(vd.at[slot], d, p_sem.at[k, 2]),
        ]

    def start(cps):
        for cp in cps:
            cp.start()

    def finish(s):
        m2, m3, m4 = s - K2, s - K3, s - K4

        def store_g():
            return [
                pltpu.make_async_copy(Gg, hgg.at[s], g_sem.at[0]),
                pltpu.make_async_copy(Gu, hgu.at[s], g_sem.at[1]),
                pltpu.make_async_copy(Gd, hgd.at[s], g_sem.at[2]),
            ]

        @when_valid(s)
        def _():
            start(store_g())

        @when_valid(m3)
        def _():
            fetched(2, 3, 4)
            add(2, 3, 4)
            start(put(2, 1, p3g.at[m3], p3u.at[m3], p3d.at[m3]))

        @when_valid(m2)
        def _():
            fetched(0, 1)
            add(0, 1)
            start(put(0, 0, p2g.at[m2], p2u.at[m2], p2d.at[m2]))

        @when_valid(m4)
        def _():
            fetched(5, 6)
            add(5, 6)
            start(outs(m4))

        @when_valid(m3)
        def _():
            for cp in put(2, 1, p3g.at[m3], p3u.at[m3], p3d.at[m3]):
                cp.wait()
            start(s3(m3))

        @when_valid(m2)
        def _():
            for cp in put(0, 0, p2g.at[m2], p2u.at[m2], p2d.at[m2]):
                cp.wait()
            start(s2(m2))

        @when_valid(s)
        def _():
            for cp in store_g():
                cp.wait()
            start(s1(s))

    DX = 4

    def dn_send():
        for b in range(DX):
            w = T // DX
            src = dn_v.at[pl.ds(pl.multiple_of(oth0 + b * w, w), w)]
            rcopy(src, dnx.at[pl.ds(b * w, w)], x_send.at[2], x_recv.at[2 + b], sib).start()

    def boundary(s):
        l = layer_of(s)

        def copies(b):
            r = pl.ds(pl.multiple_of(b * UB, UB), UB)
            k = b % 2
            return (
                pltpu.make_async_copy(h.at[l, r], st_h.at[k], st_sem.at[0, k]),
                pltpu.make_async_copy(dnx.at[r], st_dnx.at[k], st_sem.at[1, k]),
                pltpu.make_async_copy(h.at[jnp.maximum(l - 1, 0), r], st_n.at[k], st_sem.at[2, k]),
                pltpu.make_async_copy(gbuf.at[r], st_g.at[k], st_sem.at[3, k]),
            )

        def each(b, act):
            ch, cd, cn, cg = copies(b)
            act(ch)
            act(cd)

            @pl.when(l > 0)
            def _():
                act(cn)

            @pl.when(l < L - 1)
            def _():
                act(cg)

        def fetch_block(b):
            @pl.when(b % (NB // DX) == 0)
            def _():
                wait_bytes(dnx.at[pl.ds(0, T // DX)], x_recv.at[2 + b // (NB // DX)])
            each(b, lambda cp: cp.start())

        def g_out(b):
            k = b % 2
            return pltpu.make_async_copy(st_g.at[k], gbuf.at[pl.ds(pl.multiple_of(b * UB, UB), UB)], g_st.at[k])

        fetch_block(jnp.int32(0))

        def block(b, _):
            k = b % 2
            r = pl.ds(pl.multiple_of(b * UB, UB), UB)
            ro = rows(own0, b)

            @pl.when(jnp.logical_and(l > 0, b > 0))
            def _():
                g_out(b - 1).wait()

            @pl.when(b + 1 < NB)
            def _():
                fetch_block(b + 1)

            each(b, lambda cp: cp.wait())

            @pl.when(l == L - 1)
            def _():
                st_g[k] = gb_v[ro, :].astype(F32)

            rr, nf = norm_block(st_h[k].astype(F32))
            dn = dn_v[ro, :] + st_dnx[k]
            m = jnp.mean(dn * nf, axis=-1, keepdims=True)
            g = st_g[k] + rr * (dn - nf * m)
            gb_v[ro, :] = g.astype(BF16)

            @pl.when(l > 0)
            def _():
                st_g[k] = g
                g_out(b).start()
                _, nf2 = norm_block(st_n[k].astype(F32))
                n_v[ro, :] = nf2.astype(BF16)
                rcopy(gb_v.at[ro], gb_v.at[ro], x_send.at[0], x_recv.at[0], sib).start()
                rcopy(n_v.at[ro], n_v.at[ro], x_send.at[1], x_recv.at[1], sib).start()

            @pl.when(l == 0)
            def _():
                pltpu.make_async_copy(gb_v.at[ro], dh0.at[r], g_st.at[2]).start()
            return 0

        lax.fori_loop(0, NB, block, 0)
        wait_bytes(dn_v.at[half(oth0)], x_send.at[2])

        @pl.when(l > 0)
        def _():
            g_out(jnp.int32(NB - 1)).wait()
            exchange_done()

        @pl.when(l == 0)
        def _():
            wait_bytes(dh0, g_st.at[2])

    def step(s, _):
        edge = jnp.logical_and(s % NI == NI - 1, s < NT)

        @pl.when(s < 5)
        def _():
            w_relay1(2 * s + 2)
            w_relay1(2 * s + 3)

        @pl.when(s >= 5)
        def _():
            w_relay1(s + 7)

        @pl.when(jnp.logical_and(s >= 1, s < 4))
        def _():
            w_relay2(2 * s)
            w_relay2(2 * s + 1)

        @pl.when(s >= 4)
        def _():
            w_relay2(s + 4)

        begin(s)

        @when_valid(s)
        def _():
            compute(s)

        @pl.when(edge)
        def _():
            dn_send()

        finish(s)

        @pl.when(s + PF < NT)
        def _():
            @pl.when(s + PF >= WS)
            def _():
                w_drain(s + PF - WS)
            w_issue(s + PF)

        w_load(s + 1)

        @pl.when(edge)
        def _():
            boundary(s)

        w_relay_drain(s - 2)
        return 0

    lax.fori_loop(0, NT + K4 + 2, step, 0)

    def settle(s, _):
        @when_valid(s)
        def _():
            for cp in s1(s) + s2(s) + s3(s):
                cp.wait_send()
        return 0

    lax.fori_loop(0, NT, settle, 0)
    for t in range(NT - WS, NT):
        w_drain(jnp.int32(t))

    def out_done(cnt):
        wait_bytes(og.at[:, pl.ds(0, cnt)], o_recv.at[0])
        wait_bytes(ou.at[:, pl.ds(0, cnt)], o_recv.at[1])
        wait_bytes(od.at[:, pl.ds(0, cnt)], o_recv.at[2])

    @pl.when(c == 0)
    def _():
        out_done(9)

    @pl.when(c == 1)
    def _():
        out_done(10)


def call(h, gout, wgu, wd):
    A = pl.BlockSpec(memory_space=pl.ANY)
    V, S = pltpu.VMEM, pltpu.SemaphoreType
    sd = jax.ShapeDtypeStruct
    return pl.pallas_call(
        kernel,
        out_shape=(
            sd((L, NJ, 112, FC), F32), sd((L, NJ, 112, FC), F32), sd((L, NJ, 32, D), F32), sd((T, D), BF16),
            sd((L, NI, D, 2 * FC), BF16), sd((L, NI, FC, D), BF16), sd((T, D), F32), sd((T, D), F32),
            sd((NT, 4, 224, FC), F32), sd((NT, 4, 224, FC), F32), sd((NT, 8, 32, D), F32),
            sd((NT, 2, 224, FC), F32), sd((NT, 2, 224, FC), F32), sd((NT, 4, 32, D), F32),
        ) + (sd((NT, 224, FC), F32), sd((NT, 224, FC), F32), sd((NT, 2, 32, D), F32)) * 4,
        in_specs=[A] * 4,
        out_specs=(A,) * 26,
        scratch_shapes=[
            V((2 * T, D), BF16), V((2 * T, D), BF16), V((2 * T, D), F32),
            V((2, D, 2 * FC), BF16), V((2, FC, D), BF16),
            V((4, 224, FC), F32), V((4, 224, FC), F32), V((8, 32, D), F32),
            V((7, 224, FC), F32), V((7, 224, FC), F32), V((7, 2, 32, D), F32),
            V((2, UB, D), BF16), V((2, UB, D), BF16), V((2, UB, D), F32), V((2, UB, D), F32),
            S.DMA((NT, 8)), S.DMA((WS, 2, 4, 2)), S.DMA((RS, 12)), S.DMA((2,)), S.DMA((3,)), S.DMA((7, 4)), S.DMA((2, 3)),
            S.DMA((NT, 4)), S.DMA((NT, 4)), S.DMA((NT, 4)), S.DMA((NT, 4)), S.DMA((NT, 3)), S.DMA((NT, 3)),
            S.DMA((6,)), S.DMA((3,)), S.DMA((3,)), S.DMA((6,)), S.DMA((4, 2)), S.DMA((3,)),
        ],
        compiler_params=pltpu.CompilerParams(
            collective_id=0, has_side_effects=True, vmem_limit_bytes=67043328
        ),
    )(h, gout, wgu, wd)[:4]


def pack_kernel(wg, wu, out):
    for m, w in enumerate((wg, wu)):
        for j in range(NJ):
            cols = [w[0, :, 608 * d + 32 * j:608 * d + 32 * j + 32] for d in ORDER]
            out[0, j, :, FC * m:FC * m + FC] = jnp.concatenate(cols, axis=1)


def pack(wg, wu):
    return pl.pallas_call(
        pack_kernel,
        grid=(L,),
        out_shape=jax.ShapeDtypeStruct((L, NJ, 112, 2 * FC), BF16),
        in_specs=[pl.BlockSpec((1, 112, FF), lambda l: (l, 0, 0))] * 2,
        out_specs=pl.BlockSpec((1, NJ, 112, 2 * FC), lambda l: (l, 0, 0, 0)),
    )(wg, wu)


def unpack_kernel(a, b, out_a, out_b):
    for g, o in ((a, out_a), (b, out_b)):
        for t in range(FF // 128):
            parts = []
            for col in range(128 * t, 128 * t + 128, 32):
                p, j = ORDER.index(col // 608), (col % 608) // 32
                parts.append(g[0, j, :, 32 * p:32 * p + 32])
            o[0, :, 128 * t:128 * t + 128] = jnp.concatenate(parts, axis=1)


def unpack(a, b):
    rb = 56
    return pl.pallas_call(
        unpack_kernel,
        grid=(L, 112 // rb),
        out_shape=(jax.ShapeDtypeStruct((L, 112, FF), F32),) * 2,
        in_specs=[pl.BlockSpec((1, NJ, rb, FC), lambda l, r: (l, 0, r, 0))] * 2,
        out_specs=(pl.BlockSpec((1, rb, FF), lambda l, r: (l, r, 0)),) * 2,
    )(a, b)


def solution(mesh):
    tok = P(("dp", "fsdp"))
    stack = P(None, ("dp", "fsdp"))
    wsp = P(None, "fsdp")

    def local(h, gout, wg, wu, wd):
        og, ou, od, dh = call(h.reshape(L, T, D), gout.reshape(T, D), pack(wg, wu), wd.reshape(L, NJ, 32, D))
        og, ou = unpack(og, ou)
        return og, ou, od.reshape(L, 608, D), dh.reshape(1, T, D)

    return jax.shard_map(
        local, mesh=mesh, in_specs=(stack, tok, wsp, wsp, wsp), out_specs=(wsp, wsp, wsp, tok), check_vma=False
    )
```

```python
import jax
import jax.numpy as jnp
from jax import lax
from jax.experimental import pallas as pl
from jax.experimental.pallas import tpu as pltpu
from jax.sharding import PartitionSpec as P

EPS = 1e-5
MESH = pl.DeviceIdType.MESH
F32, BF16 = jnp.float32, jnp.bfloat16
L, T, D, FF = 3, 2048, 896, 4864
RW, RD = 112, 608
CW, DW = 224, 32
NJ, FC = 19, 256
FC2 = 2 * FC
NI = 10
NT = L * NI
TB, UNROLL = 512, 2
UB = 128
NB = T // UB
DX = 4
K2, K3, K4 = 3, 5, 7
PF = 8
RING = 12
SD = 4
ND = 16
ORDER = (0, 4, 2, 6, 1, 3, 5, 7)
OWN, VX, VY, DIAG = range(4)
both = jnp.logical_and


def dg(a, b, ca, cb):
    return lax.dot_general(a, b, (((ca,), (cb,)), ((), ())), preferred_element_type=F32)


def rcopy(src, dst, ss, rs, to):
    return pltpu.make_async_remote_copy(src, dst, ss, rs, device_id=to, device_id_type=MESH)


def lcopy(src, dst, sem):
    return pltpu.make_async_copy(src, dst, sem)


def wait_bytes(ref, sem):
    lcopy(ref, ref, sem).wait()


def start(cps):
    for cp in cps:
        cp.start()


def arrive(cps):
    for cp in cps:
        cp.wait_recv()


def leave(cps):
    for cp in cps:
        cp.wait_send()


def span(base, n, align):
    return pl.ds(pl.multiple_of(base, align), n)


def norm_block(xb):
    xf = xb.astype(F32)
    r = lax.rsqrt(jnp.mean(xf * xf, axis=-1, keepdims=True) + EPS)
    return r, xf * r


def kernel(h, gout, wgu, wd, og, ou, od, dh0, wbg, wbd, dnx, gbuf,
           hg, hd, h1g, h1d, p2g, p2d, h2g, h2d, p3g, p3d, h3g, h3d,
           n_v, gb_v, dn_v, wg_v, wd_v, Gg, Gd, vg, vd, st_h, st_n, st_dnx, st_g,
           w_recv, w_send, rl_send, load_sem, g_sem, v_sem, p_sem,
           s1_send, s1_recv, s2_send, s2_recv, s3_send, s3_recv,
           o_send, o_recv, gb_x, n_x, dn_send_sem, dn_recv_sem, st_sem, g_st, dh_sem):
    z, f = lax.axis_index("dp"), lax.axis_index("fsdp")
    y, x, c = f // 4, (f // 2) % 2, f % 2
    X, Y, C = 1 - x, 1 - y, 1 - c

    def dev(zz, yy, xx, cc):
        return (zz, 4 * yy + 2 * xx + cc)

    xn, yn, zn, sib = dev(z, y, X, c), dev(z, Y, x, c), dev(1 - z, y, x, c), dev(z, y, x, C)

    bar = pltpu.get_barrier_semaphore()
    for k in range(1, ND):
        o = (8 * z + f + k) % ND
        pl.semaphore_signal(bar, inc=1, device_id=(o // 8, o % 8), device_id_type=MESH)
    pl.semaphore_wait(bar, ND - 1)

    def where_of(t):
        return L - 1 - t // NI, t % NI

    def drow(yy, xx, cc):
        return span(DW * jnp.where(cc == 0, 2 * xx + yy, 4 + 2 * yy + xx), DW, DW)

    def grow(yy, xx):
        return span(CW * (2 * yy + xx), CW, 16)

    def has(t, cc):
        return both(both(t >= 0, t < NT), 2 * (t % NI) + cc < NJ)

    def primary(t):
        return t % 2 == z

    def w_sends(t, cc):
        l, i = where_of(t)
        j = 2 * i + cc
        ends = ((wgu.at[l, j], wbg.at[l, i, span(RW * f, RW, 16)]), (wd.at[l, j], wbd.at[l, i, drow(y, x, c)]))
        targets = ((dev(z, y, x, cc), cc != c), (dev(z, y, X, cc), primary(t)), (dev(z, Y, x, cc), primary(t)))
        return [
            (cond, [
                rcopy(src, dst, w_send.at[t % RING, cc, k, m], w_recv.at[t, k, m], to)
                for m, (src, dst) in enumerate(ends)
            ])
            for k, (to, cond) in enumerate(targets)
        ]

    def each_send(t, act):
        for cc in range(2):
            @pl.when(has(t, cc))
            def _():
                for cond, cps in w_sends(t, cc):
                    @pl.when(cond)
                    def _():
                        act(cps)

    def relay_to(t, yy, xx, kind, to, base):
        l, i = where_of(t)
        cuts = [(wbg, grow(yy, xx), 0)] + [(wbd, drow(yy, xx, cc), 1) for cc in range(2)]
        return [
            rcopy(b.at[l, i, r], b.at[l, i, r], rl_send.at[t % RING, base, k], w_recv.at[t, kind, m], to)
            for k, (b, r, m) in enumerate(cuts)
        ]

    def x_to_z(t):
        return relay_to(t, y, X, VX, zn, VX)

    def y_to_z(t):
        return relay_to(t, Y, x, VY, zn, VY)

    def x_to_y(t):
        return relay_to(t, y, X, DIAG, yn, OWN)

    def y_to_x(t):
        return relay_to(t, Y, x, DIAG, xn, OWN)

    def diag_to_z(t):
        return relay_to(t, Y, X, DIAG, zn, DIAG)

    def wait_kind(t, k):
        l, i = where_of(t)
        wait_bytes(wbg.at[l, i, pl.ds(0, CW)], w_recv.at[t, k, 0])
        wait_bytes(wbd.at[l, i, pl.ds(0, 2 * DW)], w_recv.at[t, k, 1])

    def when_relay(t):
        return pl.when(both(has(t, c), primary(t)))

    def w_relay1(t):
        @when_relay(t)
        def _():
            wait_kind(t, VX)
            wait_kind(t, VY)
            start(x_to_z(t) + y_to_z(t))
            by_y = (t // 2) % 2 == 0

            @pl.when(by_y)
            def _():
                start(x_to_y(t))

            @pl.when(jnp.logical_not(by_y))
            def _():
                start(y_to_x(t))

    def w_relay2(t):
        @when_relay(t)
        def _():
            wait_kind(t, DIAG)
            start(diag_to_z(t))

    def w_relay_drain(t):
        @when_relay(t)
        def _():
            leave(x_to_z(t) + y_to_z(t) + x_to_y(t) + diag_to_z(t))

    def w_load(t):
        @pl.when(has(t, c))
        def _():
            l, i = where_of(t)
            s, j = t % 2, 2 * i + c
            wait_bytes(wbg.at[l, i, pl.ds(0, RW)], w_recv.at[t, OWN, 0])
            wait_bytes(wbd.at[l, i, pl.ds(0, DW)], w_recv.at[t, OWN, 1])

            @pl.when(jnp.logical_not(primary(t)))
            def _():
                for k in (VX, VY, DIAG):
                    wait_kind(t, k)

            mine = span(RW * f, RW, 16), drow(y, x, c)
            theirs = span(RW * (f + C - c), RW, 16), drow(y, x, C)
            gs = [(wgu.at[l, j], mine[0]), (wbg.at[l, i, theirs[0]], theirs[0])]
            ds = [(wd.at[l, j], mine[1]), (wbd.at[l, i, theirs[1]], theirs[1])]
            for yy, xx in ((y, X), (Y, x), (Y, X)):
                gs.append((wbg.at[l, i, grow(yy, xx)], grow(yy, xx)))
                for cc in range(2):
                    ds.append((wbd.at[l, i, drow(yy, xx, cc)], drow(yy, xx, cc)))
            for m, (v, cuts) in enumerate(((wg_v, gs), (wd_v, ds))):
                for src, r in cuts:
                    lcopy(src, v.at[s, r], load_sem.at[m]).start()

    def w_start(lo, hi):
        for t in range(lo, hi):
            each_send(jnp.int32(t), start)

    w_start(0, 2)

    own0, oth0 = T * c, T * C
    mine, theirs = span(own0, T, T), span(oth0, T, T)

    def rows(b):
        return span(own0 + b * UB, UB, UB)

    def block_rows(b):
        return span(b * UB, UB, UB)

    def pass_rows(v, ro, sems):
        rcopy(v.at[ro], v.at[ro], sems.at[0], sems.at[1], sib).start()

    gl = lcopy(gout, gb_v.at[mine], dh_sem)
    gl.start()
    rcopy(gout, gb_v.at[mine], gb_x.at[0], gb_x.at[1], sib).start()

    def h_copy(b):
        return lcopy(h.at[L - 1, block_rows(b)], st_n.at[b % SD], st_sem.at[0, b % SD])

    for b in range(SD - 1):
        h_copy(jnp.int32(b)).start()

    def first_blocks(b, _):
        @pl.when(b + SD - 1 < NB)
        def _():
            h_copy(b + SD - 1).start()

        h_copy(b).wait()
        n_v[rows(b), :] = norm_block(st_n[b % SD])[1].astype(BF16)
        pass_rows(n_v, rows(b), n_x)
        return 0

    lax.fori_loop(0, NB, first_blocks, 0)

    def exchange_done():
        for v, sems in ((n_v, n_x), (gb_v, gb_x)):
            wait_bytes(v.at[mine], sems.at[0])
            wait_bytes(v.at[theirs], sems.at[1])

    gl.wait()
    for act, lo, hi in ((w_relay1, 2, 4), (w_relay2, 4, PF)):
        for t in range(2):
            act(jnp.int32(t))
        w_start(lo, hi)
    w_load(jnp.int32(0))
    exchange_done()

    def compute(s, hooks):
        i, ws = s % NI, s % 2
        wait_bytes(wg_v.at[ws], load_sem.at[0])
        wait_bytes(wd_v.at[ws], load_sem.at[1])
        wg, wdd = wg_v.at[ws], wd_v.at[ws]

        def block(b, _):
            for k, hook in enumerate(hooks):
                pl.when(b == k + 1)(hook)

            def load(k):
                rw = span((b * UNROLL + k) * TB, TB, TB)
                return rw, n_v[rw, :], gb_v[rw, :]

            def first(k):
                _, nb, gbb = load(k)
                return dg(nb, wg[...], 1, 0), dg(gbb, wdd[...], 1, 1)

            def middle(uv, da):
                u, v = uv[:, :FC], uv[:, FC:]
                sg = jax.nn.sigmoid(u)
                sl = u * sg
                a = (sl * v).astype(BF16)
                du = (da * v * sg * (1.0 + u * (1.0 - sg))).astype(BF16)
                dv = (da * sl).astype(BF16)
                return a, jnp.concatenate([du, dv], axis=1)

            def second(k, a, duv):
                rw, nb, gbb = load(k)
                dn_v[rw, :] = jnp.where(i == 0, 0.0, dn_v[rw, :]) + dg(duv, wg[...], 1, 1)
                g2 = dg(nb, duv, 0, 0)
                g3 = dg(a, gbb, 0, 0).reshape(Gd.shape[1:])

                def old(ref):
                    return jnp.where(b == 0, 0.0, ref[...]) if k == 0 else ref[...]

                for q in range(4):
                    part = g2[CW * q:CW * q + CW]
                    rg, ru = Gg.at[ws, 0, 2 * (q % 2) + q // 2], Gg.at[ws, 1, q]
                    rg[...] = old(rg) + part[:, :FC]
                    ru[...] = old(ru) + part[:, FC:]
                rd = Gd.at[ws]
                rd[...] = old(rd) + g3

            mids = [middle(*first(k)) for k in range(UNROLL)]
            for k in range(UNROLL):
                second(k, *mids[k])
            return 0

        lax.fori_loop(0, 2 * T // (TB * UNROLL), block, 0)

    COLORS = ((x, y, xn, yn), (y, x, yn, xn))

    def valid(s):
        return has(s, c)

    def when_valid(s):
        return pl.when(valid(s))

    def s1(s):
        return [
            rcopy(src.at[s, k, pl.ds(2 * (1 - a), 2)], dst.at[s, k], s1_send.at[s, k, m], s1_recv.at[s, k, m], to)
            for k, (a, _, to, _) in enumerate(COLORS)
            for m, (src, dst) in enumerate(((hg, h1g), (hd, h1d)))
        ]

    def s2(s):
        return [
            rcopy(src.at[s, k], dst.at[s, k], s2_send.at[s, k, m], s2_recv.at[s, k, m], to)
            for k, (_, _, _, to) in enumerate(COLORS)
            for m, (src, dst) in enumerate(((p2g, h2g), (p2d, h2d)))
        ]

    def s3(s):
        return [
            rcopy(src.at[s], dst.at[s], s3_send.at[s, m], s3_recv.at[s, m], zn)
            for m, (src, dst) in enumerate(((p3g, h3g), (p3d, h3d)))
        ]

    A0, A1, B0, B1, B2, C0, C1 = range(7)

    def outs(s):
        l, i = where_of(s)
        j = 2 * i + c
        cps = []
        for m, (cc, to) in enumerate(((c, None), (C, sib))):
            half = span(RW * cc, RW, 16)
            ends = ((vg.at[C0, 0, half], og), (vg.at[C0, 1, half], ou), (vd.at[C0, cc], od))
            for k, (src, dst) in enumerate(ends):
                sem = o_send.at[m, k]
                cps.append(rcopy(src, dst.at[l, j], sem, o_recv.at[k], to) if m else lcopy(src, dst.at[l, j], sem))
        return cps

    def fetch(slot, pick):
        for k, (a, b, _, _) in enumerate(COLORS):
            for m, (v, src) in enumerate(zip((vg, vd), pick(k, a, b))):
                lcopy(src, v.at[slot, k], v_sem.at[slot, k, m]).start()

    def add(slot, *more):
        for q in (slot, *more):
            for k in range(2):
                wait_bytes(vg.at[q, k], v_sem.at[q, k, 0])
                wait_bytes(vd.at[q, k], v_sem.at[q, k, 1])
        for r in (vg, vd):
            t = r[slot]
            for q in more:
                t = t + r[q]
            r[slot] = t

    def at(g, d, *ix):
        return g.at[ix], d.at[ix]

    def begin(tick):
        m2, m3, m4 = tick - K2, tick - K3, tick - K4

        @when_valid(m4 - 1)
        def _():
            cps = outs(m4 - 1)
            for cp in cps[:L]:
                cp.wait()
            leave(cps[L:])

        @when_valid(m4)
        def _():
            arrive(s3(m4))
            fetch(C0, lambda k, a, b: at(p3g, p3d, m4, k))
            fetch(C1, lambda k, a, b: at(h3g, h3d, m4, k))

        @when_valid(m3)
        def _():
            arrive(s2(m3))
            fetch(B0, lambda k, a, b: at(hg, hd, m3, k, 2 * a + b))
            fetch(B1, lambda k, a, b: at(h1g, h1d, m3, k, b))
            fetch(B2, lambda k, a, b: at(h2g, h2d, m3, k))

        @when_valid(m2)
        def _():
            arrive(s1(m2))
            fetch(A0, lambda k, a, b: at(hg, hd, m2, k, 2 * a + 1 - b))
            fetch(A1, lambda k, a, b: at(h1g, h1d, m2, k, 1 - b))

    def put(slot, g, d):
        return [lcopy(v.at[slot], dst, p_sem.at[slot, m]) for m, (v, dst) in enumerate(((vg, g), (vd, d)))]

    def keep(s):
        return [lcopy(v.at[s % 2], dst.at[s], g_sem.at[m]) for m, (v, dst) in enumerate(((Gg, hg), (Gd, hd)))]

    def put2(s):
        return put(A0, p2g.at[s], p2d.at[s])

    def put3(s):
        return put(B0, p3g.at[s], p3d.at[s])

    def wait_all(cps):
        for cp in cps:
            cp.wait()

    def sums(tick):
        m2, m3, m4 = tick - K2, tick - K3, tick - K4

        @when_valid(m3)
        def _():
            add(B0, B1, B2)
            start(put3(m3))

        @when_valid(m2)
        def _():
            add(A0, A1)
            start(put2(m2))

        @when_valid(m4)
        def _():
            add(C0, C1)
            start(outs(m4))

    def send_sums(tick):
        m2, m3 = tick - K2, tick - K3

        @when_valid(m3)
        def _():
            wait_all(put3(m3))
            start(s3(m3))

        @when_valid(m2)
        def _():
            wait_all(put2(m2))
            start(s2(m2))

    def send_first(s):
        @when_valid(s)
        def _():
            wait_all(keep(s))
            start(s1(s))

    def dn_send():
        w = T // DX
        for b in range(DX):
            src = dn_v.at[span(oth0 + b * w, w, w)]
            rcopy(src, dnx.at[pl.ds(b * w, w)], dn_send_sem, dn_recv_sem.at[b], sib).start()

    def boundary(s):
        l, _ = where_of(s)

        def each(b, act):
            r, k = block_rows(b), b % SD
            lower = jnp.maximum(l - 1, 0)
            cps = [
                lcopy(src, dst.at[k], st_sem.at[m, k])
                for m, (src, dst) in enumerate(((h.at[lower, r], st_n), (h.at[l, r], st_h), (dnx.at[r], st_dnx), (gbuf.at[r], st_g)))
            ]
            act(cps[1])
            act(cps[2])

            @pl.when(l > 0)
            def _():
                act(cps[0])

            @pl.when(l < L - 1)
            def _():
                act(cps[3])

        def fetch_block(b):
            per = NB // DX

            @pl.when(b % per == 0)
            def _():
                wait_bytes(dnx.at[pl.ds(0, T // DX)], dn_recv_sem.at[b // per])

            each(b, lambda cp: cp.start())

        def g_out(b):
            return lcopy(st_g.at[b % SD], gbuf.at[block_rows(b)], g_st.at[b % SD])

        for b in range(SD - 1):
            fetch_block(jnp.int32(b))

        def block(b, _):
            k, ro = b % SD, rows(b)

            @pl.when(both(l > 0, b > 0))
            def _():
                g_out(b - 1).wait()

            @pl.when(b + SD - 1 < NB)
            def _():
                fetch_block(b + SD - 1)

            each(b, lambda cp: cp.wait())

            @pl.when(l == L - 1)
            def _():
                st_g[k] = gb_v[ro, :].astype(F32)

            rr, nf = norm_block(st_h[k])
            dn = dn_v[ro, :] + st_dnx[k]
            g = st_g[k] + rr * (dn - nf * jnp.mean(dn * nf, axis=-1, keepdims=True))
            gb_v[ro, :] = g.astype(BF16)

            @pl.when(l > 0)
            def _():
                st_g[k] = g
                g_out(b).start()
                n_v[ro, :] = norm_block(st_n[k])[1].astype(BF16)
                pass_rows(gb_v, ro, gb_x)
                pass_rows(n_v, ro, n_x)

            @pl.when(l == 0)
            def _():
                lcopy(gb_v.at[ro], dh0.at[block_rows(b)], dh_sem).start()

            return 0

        lax.fori_loop(0, NB, block, 0)
        wait_bytes(dn_v.at[theirs], dn_send_sem)

        @pl.when(l > 0)
        def _():
            g_out(NB - 1).wait()
            exchange_done()

        @pl.when(l == 0)
        def _():
            wait_bytes(dh0, dh_sem)

    def is_edge(s):
        return both(s % NI == NI - 1, both(s >= 0, s < NT))

    def step(s, _):
        edge = is_edge(s)
        busy = valid(s)

        @pl.when(s < 3)
        def _():
            w_relay1(2 * s + 2)
            w_relay1(2 * s + 3)

        @pl.when(s >= 3)
        def _():
            w_relay1(s + PF - 3)

        @pl.when(both(s >= 1, s < 3))
        def _():
            w_relay2(2 * s)
            w_relay2(2 * s + 1)

        @pl.when(s >= 3)
        def _():
            w_relay2(s + 3)

        def arrivals():
            @pl.when(jnp.logical_not(is_edge(s - 1)))
            def _():
                send_first(s - 1)

            begin(s)

        def departures():
            send_sums(s)
            w_load(s + 1)

        parts = (arrivals, lambda: sums(s), departures)

        @pl.when(jnp.logical_not(busy))
        def _():
            for part in parts:
                part()

        @pl.when(busy)
        def _():
            compute(s, parts)
            start(keep(s))

        each_send(s + PF - RING, leave)
        each_send(s + PF, start)

        @pl.when(edge)
        def _():
            dn_send()
            send_first(s)
            boundary(s)

        w_relay_drain(s - 2)
        return 0

    lax.fori_loop(0, NT + K4 + 1, step, 0)

    def settle(s, _):
        @when_valid(s)
        def _():
            leave(s1(s) + s2(s) + s3(s))

        return 0

    lax.fori_loop(0, NT, settle, 0)

    def out_done(cnt):
        for k, o in enumerate((og, ou, od)):
            wait_bytes(o.at[:, pl.ds(0, cnt)], o_recv.at[k])

    for cc in range(2):
        @pl.when(c == cc)
        def _():
            out_done(NI - 1 + cc)


def call(h, gout, wgu, wd):
    A = pl.BlockSpec(memory_space=pl.ANY)
    V, S = pltpu.VMEM, pltpu.SemaphoreType
    sd = jax.ShapeDtypeStruct

    def pair(*lead):
        return (*lead, CW, FC), (*lead, DW, D)

    grads = [sd(s, F32) for lead in ((NT, 2, 4), (NT, 2, 2)) + ((NT, 2),) * 4 for s in pair(*lead)]
    return pl.pallas_call(
        kernel,
        out_shape=(
            sd((L, NJ, RW, FC), F32), sd((L, NJ, RW, FC), F32), sd((L, NJ, DW, D), F32), sd((T, D), BF16),
            sd((L, NI, D, FC2), BF16), sd((L, NI, FC, D), BF16), sd((T, D), F32), sd((T, D), F32), *grads,
        ),
        in_specs=[A] * 4,
        out_specs=(A,) * (8 + len(grads)),
        scratch_shapes=[
            V((2 * T, D), BF16), V((2 * T, D), BF16), V((2 * T, D), F32),
            V((2, D, FC2), BF16), V((2, FC, D), BF16),
            *(V(s, F32) for s in pair(2, 2, 4)), *(V(s, F32) for s in pair(7, 2)),
            *(V((SD, UB, D), t) for t in (BF16, BF16, F32, F32)),
            S.DMA((NT, 4, 2)), S.DMA((RING, 2, 3, 2)), S.DMA((RING, 4, 3)), S.DMA((2,)), S.DMA((2,)), S.DMA((7, 2, 2)), S.DMA((7, 2)),
            *(S.DMA((NT, 2, 2)) for _ in range(4)), *(S.DMA((NT, 2)) for _ in range(2)),
            S.DMA((2, 3)), S.DMA((3,)), S.DMA((2,)), S.DMA((2,)), S.DMA, S.DMA((DX,)), S.DMA((4, SD)), S.DMA((SD,)), S.DMA,
        ],
        compiler_params=pltpu.CompilerParams(
            collective_id=0, has_side_effects=True, vmem_limit_bytes=67043328
        ),
    )(h, gout, wgu, wd)[:4]


def pack_kernel(wg, wu, out):
    for m, w in enumerate((wg, wu)):
        for j in range(NJ):
            cols = [w[0, :, RD * d + DW * j:RD * d + DW * j + DW] for d in ORDER]
            out[0, j, :, FC * m:FC * m + FC] = jnp.concatenate(cols, axis=1)


def pack(wg, wu):
    return pl.pallas_call(
        pack_kernel,
        grid=(L,),
        out_shape=jax.ShapeDtypeStruct((L, NJ, RW, FC2), BF16),
        in_specs=[pl.BlockSpec((1, RW, FF), lambda l: (l, 0, 0))] * 2,
        out_specs=pl.BlockSpec((1, NJ, RW, FC2), lambda l: (l, 0, 0, 0)),
    )(wg, wu)


def unpack_kernel(a, b, d, e, out_a, out_b, out_d, out_e):
    for g, o in ((a, out_a), (b, out_b)):
        for t in range(FF // UB):
            parts = []
            for col in range(UB * t, UB * t + UB, DW):
                p, j = ORDER.index(col // RD), (col % RD) // DW
                parts.append(g[0, j, :, DW * p:DW * p + DW])
            o[0, :, UB * t:UB * t + UB] = jnp.concatenate(parts, axis=1)
    out_d[...] = d[...]
    out_e[...] = e[...]


def unpack(a, b, d, e):
    rb, db, eb = RW // 2, RD // 2, T // 4
    sd = jax.ShapeDtypeStruct
    dspec = pl.BlockSpec((1, db, D), lambda l, r: (l, r, 0))
    espec = pl.BlockSpec((eb, D), lambda l, r: (jnp.minimum(2 * l + r, 3), 0))
    return pl.pallas_call(
        unpack_kernel,
        grid=(L, 2),
        out_shape=(sd((L, RW, FF), F32), sd((L, RW, FF), F32), sd(d.shape, F32), sd(e.shape, BF16)),
        in_specs=[pl.BlockSpec((1, NJ, rb, FC), lambda l, r: (l, 0, r, 0))] * 2 + [dspec, espec],
        out_specs=(pl.BlockSpec((1, rb, FF), lambda l, r: (l, r, 0)),) * 2 + (dspec, espec),
    )(a, b, d, e)


def solution(mesh):
    tok = P(("dp", "fsdp"))
    stack = P(None, ("dp", "fsdp"))
    wsp = P(None, "fsdp")

    def local(h, gout, wg, wu, wd):
        og, ou, od, dh = call(h.reshape(L, T, D), gout.reshape(T, D), pack(wg, wu), wd.reshape(L, NJ, DW, D))
        og, ou, od, dh = unpack(og, ou, od.reshape(L, RD, D), dh)
        return og, ou, od, dh.reshape(1, T, D)

    return jax.shard_map(
        local, mesh=mesh, in_specs=(stack, tok, wsp, wsp, wsp), out_specs=(wsp, wsp, wsp, tok), check_vma=False
    )
```

```python
import jax
import jax.numpy as jnp
from jax import lax
from jax.experimental import pallas as pl
from jax.experimental.pallas import tpu as pltpu
from jax.sharding import PartitionSpec as P

EPS = 1e-5
MESH = pl.DeviceIdType.MESH
F32, BF16 = jnp.float32, jnp.bfloat16
L, T, D, FF = 3, 2048, 896, 4864
RW, RD = 112, 608
CW, DW = 224, 32
NJ, FC = 19, 256
FC2 = 2 * FC
NI = 10
NT = L * NI
LAST = NT - 1
TB, UNROLL = 512, 2
UB = 128
NB = T // UB
DX = 4
K2, K3, K4 = 3, 5, 7
PF = 8
RING = 12
SD = 4
ND = 16
ORDER = (0, 4, 2, 6, 1, 3, 5, 7)
OWN, VX, VY, DIAG = range(4)
both = jnp.logical_and


def dg(a, b, ca, cb):
    return lax.dot_general(a, b, (((ca,), (cb,)), ((), ())), preferred_element_type=F32)


def rcopy(src, dst, ss, rs, to):
    return pltpu.make_async_remote_copy(src, dst, ss, rs, device_id=to, device_id_type=MESH)


def lcopy(src, dst, sem):
    return pltpu.make_async_copy(src, dst, sem)


def wait_bytes(ref, sem):
    lcopy(ref, ref, sem).wait()


def start(cps):
    for cp in cps:
        cp.start()


def arrive(cps):
    for cp in cps:
        cp.wait_recv()


def leave(cps):
    for cp in cps:
        cp.wait_send()


def span(base, n, align):
    return pl.ds(pl.multiple_of(base, align), n)


def norm_block(xb):
    xf = xb.astype(F32)
    r = lax.rsqrt(jnp.mean(xf * xf, axis=-1, keepdims=True) + EPS)
    return r, xf * r


def kernel(h, gout, wgu, wd, og, ou, od, dh0, wbg, wbd, dnx, gbuf,
           hg, hd, h1g, h1d, p2g, p2d, h2g, h2d, p3g, p3d, h3g, h3d,
           n_v, gb_v, dn_v, wg_v, wd_v, Gg, Gd, vg, vd, st_h, st_n, st_dnx, st_g,
           w_recv, w_send, rl_send, load_sem, g_sem, v_sem, p_sem,
           s1_send, s1_recv, s2_send, s2_recv, s3_send, s3_recv,
           o_send, o_recv, gb_x, n_x, dn_send_sem, dn_recv_sem, st_sem, g_st, dh_sem):
    z, f = lax.axis_index("dp"), lax.axis_index("fsdp")
    y, x, c = f // 4, (f // 2) % 2, f % 2
    X, Y, C = 1 - x, 1 - y, 1 - c

    def dev(zz, yy, xx, cc):
        return (zz, 4 * yy + 2 * xx + cc)

    xn, yn, zn, sib = dev(z, y, X, c), dev(z, Y, x, c), dev(1 - z, y, x, c), dev(z, y, x, C)

    bar = pltpu.get_barrier_semaphore()
    for k in range(1, ND):
        o = (8 * z + f + k) % ND
        pl.semaphore_signal(bar, inc=1, device_id=(o // 8, o % 8), device_id_type=MESH)
    pl.semaphore_wait(bar, ND - 1)

    def where_of(t):
        return L - 1 - t // NI, t % NI

    def drow(yy, xx, cc):
        return span(DW * jnp.where(cc == 0, 2 * xx + yy, 4 + 2 * yy + xx), DW, DW)

    def grow(yy, xx):
        return span(CW * (2 * yy + xx), CW, 16)

    def has(t, cc):
        return both(both(t >= 0, t < NT), 2 * (t % NI) + cc < NJ)

    def primary(t):
        return t % 2 == z

    def w_sends(t, cc):
        l, i = where_of(t)
        j = 2 * i + cc
        ends = ((wgu.at[l, j], wbg.at[l, i, span(RW * f, RW, 16)]), (wd.at[l, j], wbd.at[l, i, drow(y, x, c)]))
        targets = ((dev(z, y, x, cc), cc != c), (dev(z, y, X, cc), primary(t)), (dev(z, Y, x, cc), primary(t)))
        return [
            (cond, [
                rcopy(src, dst, w_send.at[t % RING, cc, k, m], w_recv.at[t, k, m], to)
                for m, (src, dst) in enumerate(ends)
            ])
            for k, (to, cond) in enumerate(targets)
        ]

    def each_send(t, act):
        for cc in range(2):
            @pl.when(has(t, cc))
            def _():
                for cond, cps in w_sends(t, cc):
                    @pl.when(cond)
                    def _():
                        act(cps)

    def relay_to(t, yy, xx, kind, to, base):
        l, i = where_of(t)
        cuts = [(wbg, grow(yy, xx), 0)] + [(wbd, drow(yy, xx, cc), 1) for cc in range(2)]
        return [
            rcopy(b.at[l, i, r], b.at[l, i, r], rl_send.at[t % RING, base, k], w_recv.at[t, kind, m], to)
            for k, (b, r, m) in enumerate(cuts)
        ]

    def x_to_z(t):
        return relay_to(t, y, X, VX, zn, VX)

    def y_to_z(t):
        return relay_to(t, Y, x, VY, zn, VY)

    def x_to_y(t):
        return relay_to(t, y, X, DIAG, yn, OWN)

    def y_to_x(t):
        return relay_to(t, Y, x, DIAG, xn, OWN)

    def diag_to_z(t):
        return relay_to(t, Y, X, DIAG, zn, DIAG)

    def wait_kind(t, k):
        l, i = where_of(t)
        wait_bytes(wbg.at[l, i, pl.ds(0, CW)], w_recv.at[t, k, 0])
        wait_bytes(wbd.at[l, i, pl.ds(0, 2 * DW)], w_recv.at[t, k, 1])

    def when_relay(t):
        return pl.when(both(has(t, c), primary(t)))

    def w_relay1(t):
        @when_relay(t)
        def _():
            wait_kind(t, VX)
            wait_kind(t, VY)
            start(x_to_z(t) + y_to_z(t))
            by_y = (t // 2) % 2 == 0

            @pl.when(by_y)
            def _():
                start(x_to_y(t))

            @pl.when(jnp.logical_not(by_y))
            def _():
                start(y_to_x(t))

    def w_relay2(t):
        @when_relay(t)
        def _():
            wait_kind(t, DIAG)
            start(diag_to_z(t))

    def w_relay_drain(t):
        @when_relay(t)
        def _():
            leave(x_to_z(t) + y_to_z(t) + x_to_y(t) + diag_to_z(t))

    def w_load(t):
        @pl.when(has(t, c))
        def _():
            l, i = where_of(t)
            s, j = t % 2, 2 * i + c
            wait_bytes(wbg.at[l, i, pl.ds(0, RW)], w_recv.at[t, OWN, 0])
            wait_bytes(wbd.at[l, i, pl.ds(0, DW)], w_recv.at[t, OWN, 1])

            @pl.when(jnp.logical_not(primary(t)))
            def _():
                for k in (VX, VY, DIAG):
                    wait_kind(t, k)

            mine = span(RW * f, RW, 16), drow(y, x, c)
            theirs = span(RW * (f + C - c), RW, 16), drow(y, x, C)
            gs = [(wgu.at[l, j], mine[0]), (wbg.at[l, i, theirs[0]], theirs[0])]
            ds = [(wd.at[l, j], mine[1]), (wbd.at[l, i, theirs[1]], theirs[1])]
            for yy, xx in ((y, X), (Y, x), (Y, X)):
                gs.append((wbg.at[l, i, grow(yy, xx)], grow(yy, xx)))
                for cc in range(2):
                    ds.append((wbd.at[l, i, drow(yy, xx, cc)], drow(yy, xx, cc)))
            for m, (v, cuts) in enumerate(((wg_v, gs), (wd_v, ds))):
                for src, r in cuts:
                    lcopy(src, v.at[s, r], load_sem.at[m]).start()

    def w_start(lo, hi):
        for t in range(lo, hi):
            each_send(jnp.int32(t), start)

    w_start(0, 2)

    own0, oth0 = T * c, T * C
    mine, theirs = span(own0, T, T), span(oth0, T, T)

    def rows(b):
        return span(own0 + b * UB, UB, UB)

    def block_rows(b):
        return span(b * UB, UB, UB)

    def pass_rows(v, ro, sems):
        rcopy(v.at[ro], v.at[ro], sems.at[0], sems.at[1], sib).start()

    gl = lcopy(gout, gb_v.at[mine], dh_sem)
    gl.start()
    rcopy(gout, gb_v.at[mine], gb_x.at[0], gb_x.at[1], sib).start()

    def h_copy(b):
        return lcopy(h.at[L - 1, block_rows(b)], st_n.at[b % SD], st_sem.at[0, b % SD])

    for b in range(SD - 1):
        h_copy(jnp.int32(b)).start()

    def first_blocks(b, _):
        @pl.when(b + SD - 1 < NB)
        def _():
            h_copy(b + SD - 1).start()

        h_copy(b).wait()
        n_v[rows(b), :] = norm_block(st_n[b % SD])[1].astype(BF16)
        pass_rows(n_v, rows(b), n_x)
        return 0

    lax.fori_loop(0, NB, first_blocks, 0)

    def exchange_done():
        for v, sems in ((n_v, n_x), (gb_v, gb_x)):
            wait_bytes(v.at[mine], sems.at[0])
            wait_bytes(v.at[theirs], sems.at[1])

    gl.wait()
    for act, lo, hi in ((w_relay1, 2, 4), (w_relay2, 4, PF)):
        for t in range(2):
            act(jnp.int32(t))
        w_start(lo, hi)
    w_load(jnp.int32(0))
    exchange_done()

    def compute(s, hooks):
        i, ws = s % NI, s % 2
        wait_bytes(wg_v.at[ws], load_sem.at[0])
        wait_bytes(wd_v.at[ws], load_sem.at[1])
        wg, wdd = wg_v.at[ws], wd_v.at[ws]

        def block(b, _):
            for k, hook in enumerate(hooks):
                pl.when(b == k + 1)(hook)

            def load(k):
                rw = span((b * UNROLL + k) * TB, TB, TB)
                return rw, n_v[rw, :], gb_v[rw, :]

            def first(k):
                _, nb, gbb = load(k)
                return dg(nb, wg[...], 1, 0), dg(gbb, wdd[...], 1, 1)

            def middle(uv, da):
                u, v = uv[:, :FC], uv[:, FC:]
                sg = jax.nn.sigmoid(u)
                sl = u * sg
                a = (sl * v).astype(BF16)
                du = (da * v * sg * (1.0 + u * (1.0 - sg))).astype(BF16)
                dv = (da * sl).astype(BF16)
                return a, jnp.concatenate([du, dv], axis=1)

            def second(k, a, duv):
                rw, nb, gbb = load(k)
                dn_v[rw, :] = jnp.where(i == 0, 0.0, dn_v[rw, :]) + dg(duv, wg[...], 1, 1)
                g2 = dg(nb, duv, 0, 0)
                g3 = dg(a, gbb, 0, 0).reshape(Gd.shape[1:])

                def old(ref):
                    return jnp.where(b == 0, 0.0, ref[...]) if k == 0 else ref[...]

                for q in range(4):
                    part = g2[CW * q:CW * q + CW]
                    rg, ru = Gg.at[ws, 0, 2 * (q % 2) + q // 2], Gg.at[ws, 1, q]
                    rg[...] = old(rg) + part[:, :FC]
                    ru[...] = old(ru) + part[:, FC:]
                rd = Gd.at[ws]
                rd[...] = old(rd) + g3

            mids = [middle(*first(k)) for k in range(UNROLL)]
            for k in range(UNROLL):
                second(k, *mids[k])
            return 0

        lax.fori_loop(0, 2 * T // (TB * UNROLL), block, 0)

    COLORS = ((x, y, xn, yn), (y, x, yn, xn))

    def valid(s):
        return has(s, c)

    def when_valid(s):
        return pl.when(valid(s))

    def s1(s):
        return [
            rcopy(src.at[s, k, pl.ds(2 * (1 - a), 2)], dst.at[s, k], s1_send.at[s, k, m], s1_recv.at[s, k, m], to)
            for k, (a, _, to, _) in enumerate(COLORS)
            for m, (src, dst) in enumerate(((hg, h1g), (hd, h1d)))
        ]

    def s2(s):
        return [
            rcopy(src.at[s, k], dst.at[s, k], s2_send.at[s, k, m], s2_recv.at[s, k, m], to)
            for k, (_, _, _, to) in enumerate(COLORS)
            for m, (src, dst) in enumerate(((p2g, h2g), (p2d, h2d)))
        ]

    def s3(s):
        return [
            rcopy(src.at[s], dst.at[s], s3_send.at[s, m], s3_recv.at[s, m], zn)
            for m, (src, dst) in enumerate(((p3g, h3g), (p3d, h3d)))
        ]

    A0, A1, B0, B1, B2, C0, C1 = range(7)

    def outs(s):
        l, i = where_of(s)
        j = 2 * i + c
        cps = []
        for m, (cc, to) in enumerate(((c, None), (C, sib))):
            half = span(RW * cc, RW, 16)
            ends = ((vg.at[C0, 0, half], og), (vg.at[C0, 1, half], ou), (vd.at[C0, cc], od))
            for k, (src, dst) in enumerate(ends):
                sem = o_send.at[m, k]
                cps.append(rcopy(src, dst.at[l, j], sem, o_recv.at[k], to) if m else lcopy(src, dst.at[l, j], sem))
        return cps

    def fetch(slot, pick):
        for k, (a, b, _, _) in enumerate(COLORS):
            for m, (v, src) in enumerate(zip((vg, vd), pick(k, a, b))):
                lcopy(src, v.at[slot, k], v_sem.at[slot, k, m]).start()

    def add(slot, *more):
        for q in (slot, *more):
            for k in range(2):
                wait_bytes(vg.at[q, k], v_sem.at[q, k, 0])
                wait_bytes(vd.at[q, k], v_sem.at[q, k, 1])
        for r in (vg, vd):
            t = r[slot]
            for q in more:
                t = t + r[q]
            r[slot] = t

    def at(g, d, *ix):
        return g.at[ix], d.at[ix]

    def second(s):
        return jnp.where(s < LAST + K2, s - K2, jnp.where(s == LAST + K3 - 1, LAST, -1))

    def begin(tick):
        m2, m3, m4 = second(tick), tick - K3, tick - K4

        @when_valid(m4 - 1)
        def _():
            cps = outs(m4 - 1)
            for cp in cps[:L]:
                cp.wait()
            leave(cps[L:])

        @when_valid(m4)
        def _():
            arrive(s3(m4))
            fetch(C0, lambda k, a, b: at(p3g, p3d, m4, k))
            fetch(C1, lambda k, a, b: at(h3g, h3d, m4, k))

        @when_valid(m3)
        def _():
            arrive(s2(m3))
            fetch(B0, lambda k, a, b: at(hg, hd, m3, k, 2 * a + b))
            fetch(B1, lambda k, a, b: at(h1g, h1d, m3, k, b))
            fetch(B2, lambda k, a, b: at(h2g, h2d, m3, k))

        @when_valid(m2)
        def _():
            arrive(s1(m2))
            fetch(A0, lambda k, a, b: at(hg, hd, m2, k, 2 * a + 1 - b))
            fetch(A1, lambda k, a, b: at(h1g, h1d, m2, k, 1 - b))

    def put(slot, g, d):
        return [lcopy(v.at[slot], dst, p_sem.at[slot, m]) for m, (v, dst) in enumerate(((vg, g), (vd, d)))]

    def keep(s):
        return [lcopy(v.at[s % 2], dst.at[s], g_sem.at[m]) for m, (v, dst) in enumerate(((Gg, hg), (Gd, hd)))]

    def put2(s):
        return put(A0, p2g.at[s], p2d.at[s])

    def put3(s):
        return put(B0, p3g.at[s], p3d.at[s])

    def wait_all(cps):
        for cp in cps:
            cp.wait()

    def sums(tick):
        m2, m3, m4 = second(tick), tick - K3, tick - K4

        @when_valid(m3)
        def _():
            add(B0, B1, B2)
            start(put3(m3))

        @when_valid(m2)
        def _():
            add(A0, A1)
            start(put2(m2))

        @when_valid(m4)
        def _():
            add(C0, C1)
            start(outs(m4))

    def send_sums(tick):
        m2, m3 = second(tick), tick - K3

        @when_valid(m3)
        def _():
            wait_all(put3(m3))
            start(s3(m3))

        @when_valid(m2)
        def _():
            wait_all(put2(m2))
            start(s2(m2))

    def send_first(s):
        @when_valid(s)
        def _():
            wait_all(keep(s))
            start(s1(s))

    def dn_send():
        w = T // DX
        for b in range(DX):
            src = dn_v.at[span(oth0 + b * w, w, w)]
            rcopy(src, dnx.at[pl.ds(b * w, w)], dn_send_sem, dn_recv_sem.at[b], sib).start()

    def boundary(s):
        l, _ = where_of(s)

        def each(b, act):
            r, k = block_rows(b), b % SD
            lower = jnp.maximum(l - 1, 0)
            cps = [
                lcopy(src, dst.at[k], st_sem.at[m, k])
                for m, (src, dst) in enumerate(((h.at[lower, r], st_n), (h.at[l, r], st_h), (dnx.at[r], st_dnx), (gbuf.at[r], st_g)))
            ]
            act(cps[1])
            act(cps[2])

            @pl.when(l > 0)
            def _():
                act(cps[0])

            @pl.when(l < L - 1)
            def _():
                act(cps[3])

        def fetch_block(b):
            per = NB // DX

            @pl.when(b % per == 0)
            def _():
                wait_bytes(dnx.at[pl.ds(0, T // DX)], dn_recv_sem.at[b // per])

            each(b, lambda cp: cp.start())

        def g_out(b):
            return lcopy(st_g.at[b % SD], gbuf.at[block_rows(b)], g_st.at[b % SD])

        for b in range(SD - 1):
            fetch_block(jnp.int32(b))

        def block(b, _):
            k, ro = b % SD, rows(b)

            @pl.when(both(l > 0, b > 0))
            def _():
                g_out(b - 1).wait()

            @pl.when(b + SD - 1 < NB)
            def _():
                fetch_block(b + SD - 1)

            each(b, lambda cp: cp.wait())

            @pl.when(l == L - 1)
            def _():
                st_g[k] = gb_v[ro, :].astype(F32)

            rr, nf = norm_block(st_h[k])
            dn = dn_v[ro, :] + st_dnx[k]
            g = st_g[k] + rr * (dn - nf * jnp.mean(dn * nf, axis=-1, keepdims=True))
            gb_v[ro, :] = g.astype(BF16)

            @pl.when(l > 0)
            def _():
                st_g[k] = g
                g_out(b).start()
                n_v[ro, :] = norm_block(st_n[k])[1].astype(BF16)
                pass_rows(gb_v, ro, gb_x)
                pass_rows(n_v, ro, n_x)

            @pl.when(l == 0)
            def _():
                lcopy(gb_v.at[ro], dh0.at[block_rows(b)], dh_sem).start()

            return 0

        lax.fori_loop(0, NB, block, 0)
        wait_bytes(dn_v.at[theirs], dn_send_sem)

        @pl.when(l > 0)
        def _():
            g_out(NB - 1).wait()
            exchange_done()

        @pl.when(l == 0)
        def _():
            wait_bytes(dh0, dh_sem)

    def is_edge(s):
        return both(s % NI == NI - 1, both(s >= 0, s < NT))

    def step(s, _):
        edge = is_edge(s)
        busy = valid(s)

        @pl.when(s < 3)
        def _():
            w_relay1(2 * s + 2)
            w_relay1(2 * s + 3)

        @pl.when(s >= 3)
        def _():
            w_relay1(s + PF - 3)

        @pl.when(both(s >= 1, s < 3))
        def _():
            w_relay2(2 * s)
            w_relay2(2 * s + 1)

        @pl.when(s >= 3)
        def _():
            w_relay2(s + 3)

        def arrivals():
            @pl.when(jnp.logical_not(is_edge(s - 1)))
            def _():
                send_first(s - 1)

            begin(s)

        def departures():
            send_sums(s)
            w_load(s + 1)

        parts = (arrivals, lambda: sums(s), departures)

        @pl.when(jnp.logical_not(busy))
        def _():
            for part in parts:
                part()

        @pl.when(busy)
        def _():
            compute(s, parts)
            start(keep(s))

        each_send(s + PF - RING, leave)
        each_send(s + PF, start)

        @pl.when(edge)
        def _():
            dn_send()

        inner = both(edge, s < LAST)

        @pl.when(jnp.logical_or(inner, s == LAST + K2 - 1))
        def _():
            send_first(jnp.where(inner, s, LAST))

        @pl.when(jnp.logical_or(inner, s == LAST + K3))
        def _():
            boundary(jnp.where(inner, s, LAST))

        w_relay_drain(s - 2)
        return 0

    lax.fori_loop(0, NT + K4 + 1, step, 0)

    def settle(s, _):
        @when_valid(s)
        def _():
            leave(s1(s) + s2(s) + s3(s))

        return 0

    lax.fori_loop(0, NT, settle, 0)

    def out_done(cnt):
        for k, o in enumerate((og, ou, od)):
            wait_bytes(o.at[:, pl.ds(0, cnt)], o_recv.at[k])

    for cc in range(2):
        @pl.when(c == cc)
        def _():
            out_done(NI - 1 + cc)


def call(h, gout, wgu, wd):
    A = pl.BlockSpec(memory_space=pl.ANY)
    V, S = pltpu.VMEM, pltpu.SemaphoreType
    sd = jax.ShapeDtypeStruct

    def pair(*lead):
        return (*lead, CW, FC), (*lead, DW, D)

    grads = [sd(s, F32) for lead in ((NT, 2, 4), (NT, 2, 2)) + ((NT, 2),) * 4 for s in pair(*lead)]
    return pl.pallas_call(
        kernel,
        out_shape=(
            sd((L, NJ, RW, FC), F32), sd((L, NJ, RW, FC), F32), sd((L, NJ, DW, D), F32), sd((T, D), BF16),
            sd((L, NI, D, FC2), BF16), sd((L, NI, FC, D), BF16), sd((T, D), F32), sd((T, D), F32), *grads,
        ),
        in_specs=[A] * 4,
        out_specs=(A,) * (8 + len(grads)),
        scratch_shapes=[
            V((2 * T, D), BF16), V((2 * T, D), BF16), V((2 * T, D), F32),
            V((2, D, FC2), BF16), V((2, FC, D), BF16),
            *(V(s, F32) for s in pair(2, 2, 4)), *(V(s, F32) for s in pair(7, 2)),
            *(V((SD, UB, D), t) for t in (BF16, BF16, F32, F32)),
            S.DMA((NT, 4, 2)), S.DMA((RING, 2, 3, 2)), S.DMA((RING, 4, 3)), S.DMA((2,)), S.DMA((2,)), S.DMA((7, 2, 2)), S.DMA((7, 2)),
            *(S.DMA((NT, 2, 2)) for _ in range(4)), *(S.DMA((NT, 2)) for _ in range(2)),
            S.DMA((2, 3)), S.DMA((3,)), S.DMA((2,)), S.DMA((2,)), S.DMA, S.DMA((DX,)), S.DMA((4, SD)), S.DMA((SD,)), S.DMA,
        ],
        compiler_params=pltpu.CompilerParams(
            collective_id=0, has_side_effects=True, vmem_limit_bytes=67043328
        ),
    )(h, gout, wgu, wd)[:4]


def pack_kernel(wg, wu, out):
    for m, w in enumerate((wg, wu)):
        for j in range(NJ):
            cols = [w[0, :, RD * d + DW * j:RD * d + DW * j + DW] for d in ORDER]
            out[0, j, :, FC * m:FC * m + FC] = jnp.concatenate(cols, axis=1)


def pack(wg, wu):
    return pl.pallas_call(
        pack_kernel,
        grid=(L,),
        out_shape=jax.ShapeDtypeStruct((L, NJ, RW, FC2), BF16),
        in_specs=[pl.BlockSpec((1, RW, FF), lambda l: (l, 0, 0))] * 2,
        out_specs=pl.BlockSpec((1, NJ, RW, FC2), lambda l: (l, 0, 0, 0)),
    )(wg, wu)


def unpack_kernel(a, b, d, e, out_a, out_b, out_d, out_e):
    for g, o in ((a, out_a), (b, out_b)):
        for t in range(FF // UB):
            parts = []
            for col in range(UB * t, UB * t + UB, DW):
                p, j = ORDER.index(col // RD), (col % RD) // DW
                parts.append(g[0, j, :, DW * p:DW * p + DW])
            o[0, :, UB * t:UB * t + UB] = jnp.concatenate(parts, axis=1)
    out_d[...] = d[...]
    out_e[...] = e[...]


def unpack(a, b, d, e):
    rb, db, eb = RW // 2, RD // 2, T // 4
    sd = jax.ShapeDtypeStruct
    dspec = pl.BlockSpec((1, db, D), lambda l, r: (l, r, 0))
    espec = pl.BlockSpec((eb, D), lambda l, r: (jnp.minimum(2 * l + r, 3), 0))
    return pl.pallas_call(
        unpack_kernel,
        grid=(L, 2),
        out_shape=(sd((L, RW, FF), F32), sd((L, RW, FF), F32), sd(d.shape, F32), sd(e.shape, BF16)),
        in_specs=[pl.BlockSpec((1, NJ, rb, FC), lambda l, r: (l, 0, r, 0))] * 2 + [dspec, espec],
        out_specs=(pl.BlockSpec((1, rb, FF), lambda l, r: (l, r, 0)),) * 2 + (dspec, espec),
    )(a, b, d, e)


def solution(mesh):
    tok = P(("dp", "fsdp"))
    stack = P(None, ("dp", "fsdp"))
    wsp = P(None, "fsdp")

    def local(h, gout, wg, wu, wd):
        og, ou, od, dh = call(h.reshape(L, T, D), gout.reshape(T, D), pack(wg, wu), wd.reshape(L, NJ, DW, D))
        og, ou, od, dh = unpack(og, ou, od.reshape(L, RD, D), dh)
        return og, ou, od, dh.reshape(1, T, D)

    return jax.shard_map(
        local, mesh=mesh, in_specs=(stack, tok, wsp, wsp, wsp), out_specs=(wsp, wsp, wsp, tok), check_vma=False
    )
```

```python
import jax
import jax.numpy as jnp
from jax import lax
from jax.experimental import pallas as pl
from jax.experimental.pallas import tpu as pltpu
from jax.sharding import PartitionSpec as P

EPS = 1e-5
MESH = pl.DeviceIdType.MESH
F32, BF16 = jnp.float32, jnp.bfloat16
L, T, D, FF = 3, 2048, 896, 4864
RW, RD = 112, 608
CW, DW = 224, 32
NJ, FC = 19, 256
FC2 = 2 * FC
NI = 10
NT = L * NI
LAST = NT - 1
TB, UNROLL = 512, 2
UB = 128
NB = T // UB
DX = 4
K2, K3, K4 = 3, 5, 7
PF = 8
RING = 12
SD = 4
ND = 16
ORDER = (0, 4, 2, 6, 1, 3, 5, 7)
OWN, VX, VY, DIAG = range(4)
both = jnp.logical_and


def dg(a, b, ca, cb):
    return lax.dot_general(a, b, (((ca,), (cb,)), ((), ())), preferred_element_type=F32)


def rcopy(src, dst, ss, rs, to):
    return pltpu.make_async_remote_copy(src, dst, ss, rs, device_id=to, device_id_type=MESH)


def lcopy(src, dst, sem):
    return pltpu.make_async_copy(src, dst, sem)


def wait_bytes(ref, sem):
    lcopy(ref, ref, sem).wait()


def start(cps):
    for cp in cps:
        cp.start()


def wait_all(cps):
    for cp in cps:
        cp.wait()


def arrive(cps):
    for cp in cps:
        cp.wait_recv()


def leave(cps):
    for cp in cps:
        cp.wait_send()


def span(base, n, align):
    return pl.ds(pl.multiple_of(base, align), n)


def norm_block(xb):
    xf = xb.astype(F32)
    r = lax.rsqrt(jnp.mean(xf * xf, axis=-1, keepdims=True) + EPS)
    return r, xf * r


def kernel(h, gout, w_gate, w_up, wd, og, ou, od, dh0, wgu, wbg, wbd, dnx, gbuf,
           hg, hd, h1g, h1d, p2g, p2d, h2g, h2d, p3g, p3d, h3g, h3d,
           n_v, gb_v, dn_v, raw_v, packed_v, wg_v, wd_v, Gg, Gd, vg, vd, st_h, st_n, st_dnx, st_g,
           w_recv, w_send, rl_send, load_sem, g_sem, v_sem, p_sem,
           s1_send, s1_recv, s2_send, s2_recv, s3_send, s3_recv,
           o_send, o_recv, gb_x, n_x, dn_send_sem, dn_recv_sem, st_sem, g_st, dh_sem):
    z, f = lax.axis_index("dp"), lax.axis_index("fsdp")
    y, x, c = f // 4, (f // 2) % 2, f % 2
    X, Y, C = 1 - x, 1 - y, 1 - c

    def dev(zz, yy, xx, cc):
        return (zz, 4 * yy + 2 * xx + cc)

    xn, yn, zn, sib = dev(z, y, X, c), dev(z, Y, x, c), dev(1 - z, y, x, c), dev(z, y, x, C)

    bar = pltpu.get_barrier_semaphore()
    for k in range(1, ND):
        o = (8 * z + f + k) % ND
        pl.semaphore_signal(bar, inc=1, device_id=(o // 8, o % 8), device_id_type=MESH)
    pl.semaphore_wait(bar, ND - 1)

    def where_of(t):
        return L - 1 - t // NI, t % NI

    def drow(yy, xx, cc):
        return span(DW * jnp.where(cc == 0, 2 * xx + yy, 4 + 2 * yy + xx), DW, DW)

    def grow(yy, xx):
        return span(CW * (2 * yy + xx), CW, 16)

    def has(t, cc):
        return both(both(t >= 0, t < NT), 2 * (t % NI) + cc < NJ)

    def primary(t):
        return t % 2 == z

    def w_sends(t, cc):
        l, i = where_of(t)
        j = 2 * i + cc
        ends = ((wgu.at[l, j], wbg.at[l, i, span(RW * f, RW, 16)]), (wd.at[l, j], wbd.at[l, i, drow(y, x, c)]))
        targets = ((dev(z, y, x, cc), cc != c), (dev(z, y, X, cc), primary(t)), (dev(z, Y, x, cc), primary(t)))
        return [
            (cond, [
                rcopy(src, dst, w_send.at[t % RING, cc, k, m], w_recv.at[t, k, m], to)
                for m, (src, dst) in enumerate(ends)
            ])
            for k, (to, cond) in enumerate(targets)
        ]

    def each_send(t, act):
        for cc in range(2):
            @pl.when(has(t, cc))
            def _():
                for cond, cps in w_sends(t, cc):
                    @pl.when(cond)
                    def _():
                        act(cps)

    def relay_to(t, yy, xx, kind, to, base):
        l, i = where_of(t)
        cuts = [(wbg, grow(yy, xx), 0)] + [(wbd, drow(yy, xx, cc), 1) for cc in range(2)]
        return [
            rcopy(b.at[l, i, r], b.at[l, i, r], rl_send.at[t % RING, base, k], w_recv.at[t, kind, m], to)
            for k, (b, r, m) in enumerate(cuts)
        ]

    def x_to_z(t):
        return relay_to(t, y, X, VX, zn, VX)

    def y_to_z(t):
        return relay_to(t, Y, x, VY, zn, VY)

    def x_to_y(t):
        return relay_to(t, y, X, DIAG, yn, OWN)

    def y_to_x(t):
        return relay_to(t, Y, x, DIAG, xn, OWN)

    def diag_to_z(t):
        return relay_to(t, Y, X, DIAG, zn, DIAG)

    def wait_kind(t, k):
        l, i = where_of(t)
        wait_bytes(wbg.at[l, i, pl.ds(0, CW)], w_recv.at[t, k, 0])
        wait_bytes(wbd.at[l, i, pl.ds(0, 2 * DW)], w_recv.at[t, k, 1])

    def when_relay(t):
        return pl.when(both(has(t, c), primary(t)))

    def w_relay1(t):
        @when_relay(t)
        def _():
            wait_kind(t, VX)
            wait_kind(t, VY)
            start(x_to_z(t) + y_to_z(t))
            by_y = (t // 2) % 2 == 0

            @pl.when(by_y)
            def _():
                start(x_to_y(t))

            @pl.when(jnp.logical_not(by_y))
            def _():
                start(y_to_x(t))

    def w_relay2(t):
        @when_relay(t)
        def _():
            wait_kind(t, DIAG)
            start(diag_to_z(t))

    def w_relay_drain(t):
        @when_relay(t)
        def _():
            leave(x_to_z(t) + y_to_z(t) + x_to_y(t) + diag_to_z(t))

    def w_load(t):
        @pl.when(has(t, c))
        def _():
            l, i = where_of(t)
            s, j = t % 2, 2 * i + c
            wait_bytes(wbg.at[l, i, pl.ds(0, RW)], w_recv.at[t, OWN, 0])
            wait_bytes(wbd.at[l, i, pl.ds(0, DW)], w_recv.at[t, OWN, 1])

            @pl.when(jnp.logical_not(primary(t)))
            def _():
                for k in (VX, VY, DIAG):
                    wait_kind(t, k)

            mine = span(RW * f, RW, 16), drow(y, x, c)
            theirs = span(RW * (f + C - c), RW, 16), drow(y, x, C)
            gs = [(wgu.at[l, j], mine[0]), (wbg.at[l, i, theirs[0]], theirs[0])]
            ds = [(wd.at[l, j], mine[1]), (wbd.at[l, i, theirs[1]], theirs[1])]
            for yy, xx in ((y, X), (Y, x), (Y, X)):
                gs.append((wbg.at[l, i, grow(yy, xx)], grow(yy, xx)))
                for cc in range(2):
                    ds.append((wbd.at[l, i, drow(yy, xx, cc)], drow(yy, xx, cc)))
            for m, (v, cuts) in enumerate(((wg_v, gs), (wd_v, ds))):
                for src, r in cuts:
                    lcopy(src, v.at[s, r], load_sem.at[m]).start()

    def pack(l):
        cps = [lcopy(w.at[l], raw_v.at[m], st_sem.at[m, 0]) for m, w in enumerate((w_gate, w_up))]
        start(cps)
        wait_all(cps)
        for j in range(NJ):
            cols = [raw_v[m, :, RD * d + DW * j:RD * d + DW * j + DW] for m in range(2) for d in ORDER]
            packed_v[j] = jnp.concatenate(cols, axis=1)
        cp = lcopy(packed_v, wgu.at[l], st_sem.at[2, 0])
        cp.start()
        cp.wait()

    pack(L - 1)

    def w_start(lo, hi):
        for t in range(lo, hi):
            each_send(jnp.int32(t), start)

    w_start(0, 2)

    own0, oth0 = T * c, T * C
    mine, theirs = span(own0, T, T), span(oth0, T, T)

    def rows(b):
        return span(own0 + b * UB, UB, UB)

    def block_rows(b):
        return span(b * UB, UB, UB)

    def pass_rows(v, ro, sems):
        rcopy(v.at[ro], v.at[ro], sems.at[0], sems.at[1], sib).start()

    gl = lcopy(gout, gb_v.at[mine], dh_sem)
    gl.start()
    rcopy(gout, gb_v.at[mine], gb_x.at[0], gb_x.at[1], sib).start()

    def h_copy(b):
        return lcopy(h.at[L - 1, block_rows(b)], st_n.at[b % SD], st_sem.at[0, b % SD])

    for b in range(SD - 1):
        h_copy(jnp.int32(b)).start()

    def first_blocks(b, _):
        @pl.when(b + SD - 1 < NB)
        def _():
            h_copy(b + SD - 1).start()

        h_copy(b).wait()
        n_v[rows(b), :] = norm_block(st_n[b % SD])[1].astype(BF16)
        pass_rows(n_v, rows(b), n_x)
        return 0

    lax.fori_loop(0, NB, first_blocks, 0)

    def exchange_done():
        for v, sems in ((n_v, n_x), (gb_v, gb_x)):
            wait_bytes(v.at[mine], sems.at[0])
            wait_bytes(v.at[theirs], sems.at[1])

    gl.wait()
    for act, lo, hi in ((w_relay1, 2, 4), (w_relay2, 4, PF)):
        for t in range(2):
            act(jnp.int32(t))
        w_start(lo, hi)
    w_load(jnp.int32(0))
    exchange_done()

    def compute(s, hooks):
        i, ws = s % NI, s % 2
        wait_bytes(wg_v.at[ws], load_sem.at[0])
        wait_bytes(wd_v.at[ws], load_sem.at[1])
        wg, wdd = wg_v.at[ws], wd_v.at[ws]

        def block(b, _):
            for k, hook in enumerate(hooks):
                pl.when(b == k + 1)(hook)

            def load(k):
                rw = span((b * UNROLL + k) * TB, TB, TB)
                return rw, n_v[rw, :], gb_v[rw, :]

            def first(k):
                _, nb, gbb = load(k)
                return dg(nb, wg[...], 1, 0), dg(gbb, wdd[...], 1, 1)

            def middle(uv, da):
                u, v = uv[:, :FC], uv[:, FC:]
                sg = jax.nn.sigmoid(u)
                sl = u * sg
                a = (sl * v).astype(BF16)
                du = (da * v * sg * (1.0 + u * (1.0 - sg))).astype(BF16)
                dv = (da * sl).astype(BF16)
                return a, jnp.concatenate([du, dv], axis=1)

            def second(k, a, duv):
                rw, nb, gbb = load(k)
                dn_v[rw, :] = jnp.where(i == 0, 0.0, dn_v[rw, :]) + dg(duv, wg[...], 1, 1)
                g2 = dg(nb, duv, 0, 0)
                g3 = dg(a, gbb, 0, 0).reshape(Gd.shape[1:])

                def old(ref):
                    return jnp.where(b == 0, 0.0, ref[...]) if k == 0 else ref[...]

                for q in range(4):
                    part = g2[CW * q:CW * q + CW]
                    rg, ru = Gg.at[ws, 0, 2 * (q % 2) + q // 2], Gg.at[ws, 1, q]
                    rg[...] = old(rg) + part[:, :FC]
                    ru[...] = old(ru) + part[:, FC:]
                rd = Gd.at[ws]
                rd[...] = old(rd) + g3

            mids = [middle(*first(k)) for k in range(UNROLL)]
            for k in range(UNROLL):
                second(k, *mids[k])
            return 0

        lax.fori_loop(0, 2 * T // (TB * UNROLL), block, 0)

    COLORS = ((x, y, xn, yn), (y, x, yn, xn))

    def valid(s):
        return has(s, c)

    def when_valid(s):
        return pl.when(valid(s))

    def s1(s):
        return [
            rcopy(src.at[s, k, pl.ds(2 * (1 - a), 2)], dst.at[s, k], s1_send.at[s, k, m], s1_recv.at[s, k, m], to)
            for k, (a, _, to, _) in enumerate(COLORS)
            for m, (src, dst) in enumerate(((hg, h1g), (hd, h1d)))
        ]

    def s2(s):
        return [
            rcopy(src.at[s, k], dst.at[s, k], s2_send.at[s, k, m], s2_recv.at[s, k, m], to)
            for k, (_, _, _, to) in enumerate(COLORS)
            for m, (src, dst) in enumerate(((p2g, h2g), (p2d, h2d)))
        ]

    def s3(s):
        return [
            rcopy(src.at[s], dst.at[s], s3_send.at[s, m], s3_recv.at[s, m], zn)
            for m, (src, dst) in enumerate(((p3g, h3g), (p3d, h3d)))
        ]

    A0, A1, B0, B1, B2, C0, C1 = range(7)

    def outs(s):
        l, i = where_of(s)
        j = 2 * i + c
        cps = []
        for m, (cc, to) in enumerate(((c, None), (C, sib))):
            half = span(RW * cc, RW, 16)
            ends = ((vg.at[C0, 0, half], og), (vg.at[C0, 1, half], ou), (vd.at[C0, cc], od))
            for k, (src, dst) in enumerate(ends):
                sem = o_send.at[m, k]
                cps.append(rcopy(src, dst.at[l, j], sem, o_recv.at[k], to) if m else lcopy(src, dst.at[l, j], sem))
        return cps

    def fetch(slot, pick):
        for k, (a, b, _, _) in enumerate(COLORS):
            for m, (v, src) in enumerate(zip((vg, vd), pick(k, a, b))):
                lcopy(src, v.at[slot, k], v_sem.at[slot, k, m]).start()

    def add(slot, *more):
        for q in (slot, *more):
            for k in range(2):
                wait_bytes(vg.at[q, k], v_sem.at[q, k, 0])
                wait_bytes(vd.at[q, k], v_sem.at[q, k, 1])
        for r in (vg, vd):
            t = r[slot]
            for q in more:
                t = t + r[q]
            r[slot] = t

    def at(g, d, *ix):
        return g.at[ix], d.at[ix]

    def second(s):
        return jnp.where(s < LAST + K2, s - K2, jnp.where(s == LAST + K3 - 1, LAST, -1))

    def begin(tick):
        m2, m3, m4 = second(tick), tick - K3, tick - K4

        @when_valid(m4 - 1)
        def _():
            cps = outs(m4 - 1)
            for cp in cps[:L]:
                cp.wait()
            leave(cps[L:])

        @when_valid(m4)
        def _():
            arrive(s3(m4))
            fetch(C0, lambda k, a, b: at(p3g, p3d, m4, k))
            fetch(C1, lambda k, a, b: at(h3g, h3d, m4, k))

        @when_valid(m3)
        def _():
            arrive(s2(m3))
            fetch(B0, lambda k, a, b: at(hg, hd, m3, k, 2 * a + b))
            fetch(B1, lambda k, a, b: at(h1g, h1d, m3, k, b))
            fetch(B2, lambda k, a, b: at(h2g, h2d, m3, k))

        @when_valid(m2)
        def _():
            arrive(s1(m2))
            fetch(A0, lambda k, a, b: at(hg, hd, m2, k, 2 * a + 1 - b))
            fetch(A1, lambda k, a, b: at(h1g, h1d, m2, k, 1 - b))

    def put(slot, g, d):
        return [lcopy(v.at[slot], dst, p_sem.at[slot, m]) for m, (v, dst) in enumerate(((vg, g), (vd, d)))]

    def keep(s):
        return [lcopy(v.at[s % 2], dst.at[s], g_sem.at[m]) for m, (v, dst) in enumerate(((Gg, hg), (Gd, hd)))]

    def put2(s):
        return put(A0, p2g.at[s], p2d.at[s])

    def put3(s):
        return put(B0, p3g.at[s], p3d.at[s])

    def sums(tick):
        m2, m3, m4 = second(tick), tick - K3, tick - K4

        @when_valid(m3)
        def _():
            add(B0, B1, B2)
            start(put3(m3))

        @when_valid(m2)
        def _():
            add(A0, A1)
            start(put2(m2))

        @when_valid(m4)
        def _():
            add(C0, C1)
            start(outs(m4))

    def send_sums(tick):
        m2, m3 = second(tick), tick - K3

        @when_valid(m3)
        def _():
            wait_all(put3(m3))
            start(s3(m3))

        @when_valid(m2)
        def _():
            wait_all(put2(m2))
            start(s2(m2))

    def send_first(s):
        @when_valid(s)
        def _():
            wait_all(keep(s))
            start(s1(s))

    def dn_send():
        w = T // DX
        for b in range(DX):
            src = dn_v.at[span(oth0 + b * w, w, w)]
            rcopy(src, dnx.at[pl.ds(b * w, w)], dn_send_sem, dn_recv_sem.at[b], sib).start()

    def boundary(s):
        l, _ = where_of(s)

        def each(b, act):
            r, k = block_rows(b), b % SD
            lower = jnp.maximum(l - 1, 0)
            cps = [
                lcopy(src, dst.at[k], st_sem.at[m, k])
                for m, (src, dst) in enumerate(((h.at[lower, r], st_n), (h.at[l, r], st_h), (dnx.at[r], st_dnx), (gbuf.at[r], st_g)))
            ]
            act(cps[1])
            act(cps[2])

            @pl.when(l > 0)
            def _():
                act(cps[0])

            @pl.when(l < L - 1)
            def _():
                act(cps[3])

        def fetch_block(b):
            per = NB // DX

            @pl.when(b % per == 0)
            def _():
                wait_bytes(dnx.at[pl.ds(0, T // DX)], dn_recv_sem.at[b // per])

            each(b, lambda cp: cp.start())

        def g_out(b):
            return lcopy(st_g.at[b % SD], gbuf.at[block_rows(b)], g_st.at[b % SD])

        for b in range(SD - 1):
            fetch_block(jnp.int32(b))

        def block(b, _):
            k, ro = b % SD, rows(b)

            @pl.when(both(l > 0, b > 0))
            def _():
                g_out(b - 1).wait()

            @pl.when(b + SD - 1 < NB)
            def _():
                fetch_block(b + SD - 1)

            each(b, lambda cp: cp.wait())

            @pl.when(l == L - 1)
            def _():
                st_g[k] = gb_v[ro, :].astype(F32)

            rr, nf = norm_block(st_h[k])
            dn = dn_v[ro, :] + st_dnx[k]
            g = st_g[k] + rr * (dn - nf * jnp.mean(dn * nf, axis=-1, keepdims=True))
            gb_v[ro, :] = g.astype(BF16)

            @pl.when(l > 0)
            def _():
                st_g[k] = g
                g_out(b).start()
                n_v[ro, :] = norm_block(st_n[k])[1].astype(BF16)
                pass_rows(gb_v, ro, gb_x)
                pass_rows(n_v, ro, n_x)

            @pl.when(l == 0)
            def _():
                lcopy(gb_v.at[ro], dh0.at[block_rows(b)], dh_sem).start()

            return 0

        lax.fori_loop(0, NB, block, 0)
        wait_bytes(dn_v.at[theirs], dn_send_sem)

        @pl.when(l > 0)
        def _():
            g_out(NB - 1).wait()
            exchange_done()

        @pl.when(l == 0)
        def _():
            wait_bytes(dh0, dh_sem)

    def is_edge(s):
        return both(s % NI == NI - 1, both(s >= 0, s < NT))

    def step(s, _):
        edge = is_edge(s)
        busy = valid(s)

        pack_at = both(s % 2 == 1, s < 2 * L - 2)

        @pl.when(pack_at)
        def _():
            pack(L - 2 - s // 2)

        @pl.when(s < 3)
        def _():
            w_relay1(2 * s + 2)
            w_relay1(2 * s + 3)

        @pl.when(s >= 3)
        def _():
            w_relay1(s + PF - 3)

        @pl.when(both(s >= 1, s < 3))
        def _():
            w_relay2(2 * s)
            w_relay2(2 * s + 1)

        @pl.when(s >= 3)
        def _():
            w_relay2(s + 3)

        def arrivals():
            @pl.when(jnp.logical_not(is_edge(s - 1)))
            def _():
                send_first(s - 1)

            begin(s)

        def departures():
            send_sums(s)
            w_load(s + 1)

        parts = (arrivals, lambda: sums(s), departures)

        @pl.when(jnp.logical_not(busy))
        def _():
            for part in parts:
                part()

        @pl.when(busy)
        def _():
            compute(s, parts)
            start(keep(s))

        each_send(s + PF - RING, leave)
        each_send(s + PF, start)

        @pl.when(edge)
        def _():
            dn_send()

        inner = both(edge, s < LAST)

        @pl.when(jnp.logical_or(inner, s == LAST + K2 - 1))
        def _():
            send_first(jnp.where(inner, s, LAST))

        @pl.when(jnp.logical_or(inner, s == LAST + K3))
        def _():
            boundary(jnp.where(inner, s, LAST))

        w_relay_drain(s - 2)
        return 0

    lax.fori_loop(0, NT + K4 + 1, step, 0)

    def settle(s, _):
        @when_valid(s)
        def _():
            leave(s1(s) + s2(s) + s3(s))

        return 0

    lax.fori_loop(0, NT, settle, 0)

    def out_done(cnt):
        for k, o in enumerate((og, ou, od)):
            wait_bytes(o.at[:, pl.ds(0, cnt)], o_recv.at[k])

    for cc in range(2):
        @pl.when(c == cc)
        def _():
            out_done(NI - 1 + cc)


def call(h, gout, wg, wu, wd):
    A = pl.BlockSpec(memory_space=pl.ANY)
    V, S = pltpu.VMEM, pltpu.SemaphoreType
    sd = jax.ShapeDtypeStruct

    def pair(*lead):
        return (*lead, CW, FC), (*lead, DW, D)

    grads = [sd(s, F32) for lead in ((NT, 2, 4), (NT, 2, 2)) + ((NT, 2),) * 4 for s in pair(*lead)]
    return pl.pallas_call(
        kernel,
        out_shape=(
            sd((L, NJ, RW, FC), F32), sd((L, NJ, RW, FC), F32), sd((L, NJ, DW, D), F32), sd((T, D), BF16),
            sd((L, NJ, RW, FC2), BF16), sd((L, NI, D, FC2), BF16), sd((L, NI, FC, D), BF16), sd((T, D), F32), sd((T, D), F32), *grads,
        ),
        in_specs=[A] * 5,
        out_specs=(A,) * (9 + len(grads)),
        scratch_shapes=[
            V((2 * T, D), BF16), V((2 * T, D), BF16), V((2 * T, D), F32),
            V((2, RW, FF), BF16), V((NJ, RW, FC2), BF16), V((2, D, FC2), BF16), V((2, FC, D), BF16),
            *(V(s, F32) for s in pair(2, 2, 4)), *(V(s, F32) for s in pair(7, 2)),
            *(V((SD, UB, D), t) for t in (BF16, BF16, F32, F32)),
            S.DMA((NT, 4, 2)), S.DMA((RING, 2, 3, 2)), S.DMA((RING, 4, 3)), S.DMA((2,)), S.DMA((2,)), S.DMA((7, 2, 2)), S.DMA((7, 2)),
            *(S.DMA((NT, 2, 2)) for _ in range(4)), *(S.DMA((NT, 2)) for _ in range(2)),
            S.DMA((2, 3)), S.DMA((3,)), S.DMA((2,)), S.DMA((2,)), S.DMA, S.DMA((DX,)), S.DMA((4, SD)), S.DMA((SD,)), S.DMA,
        ],
        compiler_params=pltpu.CompilerParams(
            collective_id=0, has_side_effects=True, vmem_limit_bytes=67043328
        ),
    )(h, gout, wg, wu, wd)[:4]


def unpack_kernel(a, b, d, e, out_a, out_b, out_d, out_e):
    for g, o in ((a, out_a), (b, out_b)):
        for t in range(FF // UB):
            parts = []
            for col in range(UB * t, UB * t + UB, DW):
                p, j = ORDER.index(col // RD), (col % RD) // DW
                parts.append(g[0, j, :, DW * p:DW * p + DW])
            o[0, :, UB * t:UB * t + UB] = jnp.concatenate(parts, axis=1)
    out_d[...] = d[...]
    out_e[...] = e[...]


def unpack(a, b, d, e):
    rb, db, eb = RW // 2, RD // 2, T // 4
    sd = jax.ShapeDtypeStruct
    dspec = pl.BlockSpec((1, db, D), lambda l, r: (l, r, 0))
    espec = pl.BlockSpec((eb, D), lambda l, r: (jnp.minimum(2 * l + r, 3), 0))
    return pl.pallas_call(
        unpack_kernel,
        grid=(L, 2),
        out_shape=(sd((L, RW, FF), F32), sd((L, RW, FF), F32), sd(d.shape, F32), sd(e.shape, BF16)),
        in_specs=[pl.BlockSpec((1, NJ, rb, FC), lambda l, r: (l, 0, r, 0))] * 2 + [dspec, espec],
        out_specs=(pl.BlockSpec((1, rb, FF), lambda l, r: (l, r, 0)),) * 2 + (dspec, espec),
    )(a, b, d, e)


def solution(mesh):
    tok = P(("dp", "fsdp"))
    stack = P(None, ("dp", "fsdp"))
    wsp = P(None, "fsdp")

    def local(h, gout, wg, wu, wd):
        og, ou, od, dh = call(h.reshape(L, T, D), gout.reshape(T, D), wg, wu, wd.reshape(L, NJ, DW, D))
        og, ou, od, dh = unpack(og, ou, od.reshape(L, RD, D), dh)
        return og, ou, od, dh.reshape(1, T, D)

    return jax.shard_map(
        local, mesh=mesh, in_specs=(stack, tok, wsp, wsp, wsp), out_specs=(wsp, wsp, wsp, tok), check_vma=False
    )
```
